512 devices in a mesh: gz: 16 (over z_lo, core), gy: 8 (over y, z_hi), gx: 4 (over x).
Axes of the slice: x: 4, y: 4, z: 16 (z_hi: 2, z_lo: 8; z = z_hi * 8 + z_lo), core: 2. Of those that a mesh axis runs over, the one named last changes fastest.
Arguments:
- velocity: float32 [3, 128, 128, 2048], P(None, 'gx', 'gy', 'gz'), may hold values from -3.5 to 5.5
- pressure: float32 [128, 128, 2048], P('gx', 'gy', 'gz'), may hold values from -6 to 6
- voidage: float32 [128, 128, 2048], P('gx', 'gy', 'gz'), may hold values from 0.5 to 0.95
- particle_vel: float32 [3, 128, 128, 2048], P(None, 'gx', 'gy', 'gz'), may hold values from -6 to 6
- forcing: float32 [1], replicated, may hold values from 0.5 to 2
- target_flux: float32 [1], replicated, may hold values from 0.5 to 1.5
Outputs:
- vel_new: float32 [3, 128, 128, 2048], P(None, 'gx', 'gy', 'gz')
- source: float32 [128, 128, 2048], P('gx', 'gy', 'gz')
- forcing_new: float32 [1], replicated
The draws below stay inside these ranges and needn't reach their ends.
All inputs are finite; a program needn't handle non-finite values.
Results may differ from the reference program's by a relative error of at most 0.000079.
Values sent between devices are 32-bit elements; how exact they have to be, the bound alone decides.
A program may use at most 64 MiB of HBM per device.

```python
import jax
import jax.numpy as jnp
from jax import lax

NX = 128
NY = 128
NZ = 2048


def draw_velocity(key, part):
    jitter_field = jnp.clip(jax.random.normal(key, (3, NX, NY, NZ), jnp.float32), -3.5, 3.5)
    mean_lift = 2.0
    upward_mask = (jnp.arange(3) == 2).astype(jnp.float32).reshape(3, 1, 1, 1)
    return (jitter_field + mean_lift * upward_mask).astype(jnp.float32)


def levels(stream_key, shape, split, low, top_value):
    factor_of = 1.0
    for dim, shards_of in split:
        draws = jax.random.uniform(jax.random.fold_in(jax.random.fold_in(stream_key, 6), dim), (shards_of,), jnp.float32, low / len(split), top_value / len(split))
        factor_of = factor_of * jnp.repeat(jnp.exp(draws), shape[dim] // shards_of).reshape((-1,) + (1,) * (len(shape) - 1 - dim))
    return factor_of


def noise(key, extent, deviation, reach, split=(), kind=jnp.bfloat16):
    result = jax.random.normal(key, extent, jnp.float32) * deviation
    if len(split) > 0:
        result = levels(key, extent, split, -0.22, 0.18) * result
    return jnp.clip(result, min=-reach, max=reach).astype(kind)


def setup_inputs(seed: int = 0) -> dict:
    seeds = jax.random.split(jax.random.key(seed), 7)
    velocity = draw_velocity(jax.random.fold_in(seeds[6], 71), 0)
    pressure = noise(seeds[1], (NX, NY, NZ), 1.0, 6.0, ((0, 4), (1, 8), (2, 16)), jnp.float32)
    voidage = jnp.clip(0.5 + 0.45 * jax.random.uniform(seeds[2], (NX, NY, NZ), jnp.float32) ** levels(seeds[2], (NX, NY, NZ), ((0, 4), (1, 8), (2, 16)), -0.2, 0.2), 0.5, 0.95)
    particle_vel = noise(seeds[3], (3, NX, NY, NZ), 1.0, 6.0, ((1, 4), (2, 8), (3, 16)), jnp.float32)
    forcing = jnp.clip(jax.random.uniform(seeds[4], (1,), jnp.float32, 0.5, 2.0), 0.5, 2.0)
    target_flux = jnp.clip(jax.random.uniform(seeds[5], (1,), jnp.float32, 0.5, 1.5), 0.5, 1.5)
    return {"velocity": velocity, "pressure": pressure, "voidage": voidage, "particle_vel": particle_vel, "forcing": forcing, "target_flux": target_flux}


time_step = 0.2
viscosity = 0.1
drag_scale = 1.0

def shifted(field, axis_no, offset):
    slices = [slice(1, -1)] * 3
    length = field.shape[field.ndim - 3 + axis_no]
    slices[axis_no] = slice(1 + offset, length - 1 + offset)
    return field[tuple([slice(None)] * (field.ndim - 3) + slices)]

def upward():
    return (jnp.arange(3) == 2).astype(jnp.float32).reshape(3, 1, 1, 1)

def predict(vel_pad, pres_pad, voidage, particle_vel, forcing):
    centre = shifted(vel_pad, 0, 0)
    advection = jnp.zeros_like(centre)
    laplace = -6.0 * centre
    grads = []
    for axis_no in range(3):
        upper = shifted(vel_pad, axis_no, 1)
        lower = shifted(vel_pad, axis_no, -1)
        advection = advection + centre[axis_no] * (upper - lower) * 0.5
        laplace = laplace + upper + lower
        grads.append((shifted(pres_pad, axis_no, 1) - shifted(pres_pad, axis_no, -1)) * 0.5)
    forces = -advection + viscosity * laplace - jnp.stack(grads) + forcing * upward()
    slip_speed = jnp.sqrt(lax.optimization_barrier(jnp.sum((centre - particle_vel) ** 2, axis=0)))
    drag_rate = drag_scale * (1.0 - voidage) * voidage ** (-2.65) * (1.0 + slip_speed)
    return (centre + time_step * (forces + drag_rate * particle_vel)) / (1.0 + time_step * drag_rate)

def reference(velocity, pressure, voidage, particle_vel, forcing, target_flux):
    vel_pad = jnp.pad(velocity, ((0, 0), (1, 1), (1, 1), (0, 0)))
    vel_pad = jnp.pad(vel_pad, ((0, 0), (0, 0), (0, 0), (1, 1)), mode='wrap')
    pres_pad = jnp.pad(pressure, ((0, 0), (0, 0), (1, 1)), mode='wrap')
    pres_pad = jnp.pad(pres_pad, ((1, 1), (1, 1), (0, 0)), mode='edge')
    ustar = predict(vel_pad, pres_pad, voidage, particle_vel, forcing[0])
    flow_sum = jnp.sum(voidage * ustar[2])
    void_sum = jnp.sum(voidage)
    cells = voidage.size
    force_step = (target_flux[0] * cells - flow_sum) / (time_step * void_sum)
    vel_new = ustar + time_step * force_step * upward()
    flux = voidage * vel_new
    flux_pad = jnp.pad(flux, ((0, 0), (1, 1), (1, 1), (0, 0)))
    flux_pad = jnp.pad(flux_pad, ((0, 0), (0, 0), (0, 0), (1, 1)), mode='wrap')
    source = jnp.zeros_like(voidage)
    for axis_no in range(3):
        source = source + (shifted(flux_pad[axis_no], axis_no, 1) - shifted(flux_pad[axis_no], axis_no, -1)) * 0.5
    return (vel_new, source, forcing + force_step)
```

```python
import jax
import jax.numpy as jnp
from jax import lax
from jax.experimental import pallas as pl
from jax.experimental.pallas import tpu as pltpu
from jax.sharding import PartitionSpec as P

MESH = pl.DeviceIdType.MESH
DT = 0.2
NU = 0.1
BX, BY, BZ = 32, 16, 128
ROWS = BX * BY
PAD = ROWS + 2 * BY
VX, VY, VZ, PR = 0, 1, 2, 3
FVZ, FVY, FP, FVX, FD, FC = 0, 1, 2, 3, 4, 5


def kernel(
    force_ref, target_ref, vel_h, pres_h, eps_h, pv_h,
    vel_o, src_o, force_o,
    V, E, PV, G, S, SL, FX, Q,
    xrecv, zsend, zrecv, zsend2, zrecv2, ysend, yrecv, xsend2,
    row1, red1, row2, red2,
    lsem, xs, xr, zs, zr, zs2, zr2, ys, yr, xs2, xr2, s1, r1, s2, r2,
):
    gz, gy, gx = lax.axis_index("gz"), lax.axis_index("gy"), lax.axis_index("gx")
    ngz, ngy, ngx = 16, 8, 4
    here = {"gz": gz, "gy": gy, "gx": gx}

    def at(**kw):
        return {**here, **kw}

    y, zhi = gy // 2, gy % 2
    zlo, core = gz // 2, gz % 2
    zabs = zhi * 8 + zlo
    xi, yi = gx, y
    has_xlo, has_xhi = gx > 0, gx < ngx - 1
    has_ylo, has_yhi = gy > 0, gy < ngy - 1

    def of_z(z):
        return at(gz=lax.rem(z, 8) * 2 + core, gy=y * 2 + z // 8)

    def of_plane(i):
        return at(gx=i // 8, gy=lax.rem(i // 2, 4) * 2 + zhi, gz=zlo * 2 + lax.rem(i, 2))

    plane = gx * 8 + y * 2 + core
    zpeers = [of_z(lax.rem(zabs + k, 16)) for k in range(1, 16)]
    ppeers = [of_plane(lax.rem(plane + k, 32)) for k in range(1, 32)]
    zlow, zhigh = at(gz=lax.rem(gz + ngz - 1, ngz)), at(gz=lax.rem(gz + 1, ngz))
    ylow, yhigh = at(gy=lax.rem(gy + ngy - 1, ngy)), at(gy=lax.rem(gy + 1, ngy))
    xlow, xhigh = at(gx=lax.rem(gx + ngx - 1, ngx)), at(gx=lax.rem(gx + 1, ngx))

    barrier = pltpu.get_barrier_semaphore()
    partners = [ylow, yhigh] + zpeers + [zlow, zhigh] + ppeers
    for d in partners:
        pl.semaphore_signal(barrier, inc=1, device_id=d, device_id_type=MESH)

    loads = [
        pltpu.make_async_copy(vel_h, V.at[pl.ds(0, 3), pl.ds(BY, ROWS), :], lsem.at[0]),
        pltpu.make_async_copy(pres_h, V.at[3, pl.ds(BY, ROWS), :], lsem.at[1]),
        pltpu.make_async_copy(eps_h, E, lsem.at[2]),
        pltpu.make_async_copy(pv_h, PV, lsem.at[3]),
    ]
    for cp in loads:
        cp.start()

    lane = lax.broadcasted_iota(jnp.int32, (BY, BZ), 1)
    rown = lax.broadcasted_iota(jnp.int32, (BY, BZ), 0)
    zero = jnp.zeros((BY, BZ), jnp.float32)
    for f in range(4):
        V[f, pl.ds(0, BY), :] = zero
        V[f, pl.ds(ROWS + BY, BY), :] = zero
    Q[...] = jnp.zeros_like(Q)
    force = force_ref[0]
    for cp in loads:
        cp.wait()

    def face(side):
        return 0 if side == 0 else BY - 1

    for side in range(2):
        for slot, f in ((FVZ, VZ), (FVY, VY), (FP, PR), (FVX, VX)):
            ysend[side, slot] = V[f, pl.ds(BY + face(side), BX, stride=BY), :]

    def slab(x, carry):
        o = pl.multiple_of(x * BY, BY)
        c = [V[f, pl.ds(o + BY, BY), :] for f in range(4)]
        xm = [V[f, pl.ds(o, BY), :] for f in range(4)]
        xp = [V[f, pl.ds(o + 2 * BY, BY), :] for f in range(4)]
        e = E[pl.ds(o, BY), :]
        pv = [PV[k, pl.ds(o, BY), :] for k in range(3)]
        zm = [jnp.where(lane == 0, 0.0, pltpu.roll(a, 1, 1)) for a in c]
        zp = [jnp.where(lane == BZ - 1, 0.0, pltpu.roll(a, BZ - 1, 1)) for a in c]
        ym = [jnp.where(rown == 0, 0.0, pltpu.roll(a, 1, 0)) for a in c]
        yp = [jnp.where(rown == BY - 1, 0.0, pltpu.roll(a, BY - 1, 0)) for a in c]
        slip = jnp.sqrt(
            (c[0] - pv[0]) * (c[0] - pv[0])
            + (c[1] - pv[1]) * (c[1] - pv[1])
            + (c[2] - pv[2]) * (c[2] - pv[2])
        )
        drag = (1.0 - e) * jnp.exp(-2.65 * jnp.log(e)) * (1.0 + slip)
        w = 1.0 / (1.0 + DT * drag)
        hi, lo = (xp, yp, zp), (xm, ym, zm)
        for k in range(3):
            adv = zero
            lap = -6.0 * c[k]
            for d in range(3):
                adv = adv + c[d] * (hi[d][k] - lo[d][k])
                lap = lap + hi[d][k] + lo[d][k]
            fk = NU * lap - 0.5 * (adv + (hi[k][3] - lo[k][3]))
            if k == 2:
                fk = fk + force
            vel_o[k, pl.ds(o, BY), :] = (c[k] + DT * (fk + drag * pv[k])) * w
        G[pl.ds(o, BY), :] = DT * w
        s = zero
        for k, a in enumerate(c + [e]):
            s = jnp.where(lane == k, a if k == 0 else pltpu.roll(a, k, 1), s)
            s = jnp.where(lane == 8 + k, pltpu.roll(a, 9 + k, 1), s)
        S[pl.ds(o, BY), :] = s
        return carry

    lax.fori_loop(0, BX, slab, 0)

    def pack(dst):
        for i in range(4):
            t = S[pl.ds(BZ * i, BZ), :].T
            dst[0, :, pl.ds(BZ * i, BZ)] = t[0:8]
            dst[1, :, pl.ds(BZ * i, BZ)] = t[8:16]

    pack(zsend)
    for side in range(2):
        ysend[side, FD] = (
            E[pl.ds(face(side), BX, stride=BY), :] * G[pl.ds(face(side), BX, stride=BY), :]
        )

    pl.semaphore_wait(barrier, len(partners))

    def remote(src, dst, a, b, dev):
        return pltpu.make_async_remote_copy(
            src_ref=src, dst_ref=dst, send_sem=a, recv_sem=b, device_id=dev, device_id_type=MESH
        )

    def ycopy(side, f):
        return remote(
            ysend.at[side, f], yrecv.at[1 - side, f], ys.at[side, f], yr.at[1 - side, f],
            ylow if side == 0 else yhigh,
        )

    def yhas(side):
        return has_ylo if side == 0 else has_yhi

    def xcopy(side):
        r = BY if side == 0 else ROWS
        return remote(
            V.at[:, pl.ds(r, BY), :], xrecv.at[1 - side], xs.at[side], xr.at[1 - side],
            xlow if side == 0 else xhigh,
        )

    def xhas(side):
        return has_xlo if side == 0 else has_xhi

    def zcopy(side, src, dst, a, b):
        return remote(
            src.at[side], dst.at[1 - side], a.at[side], b.at[1 - side],
            zlow if side == 0 else zhigh,
        )

    def when_each(has, fn):
        for side in range(2):
            pl.when(has(side))(lambda side=side: fn(side))

    def send_y(side, fields):
        for f in fields:
            ycopy(side, f).start()

    when_each(yhas, lambda side: send_y(side, (FVZ,)))
    for side in range(2):
        zcopy(side, zsend, zrecv, zs, zr).start()
    when_each(xhas, lambda side: xcopy(side).start())
    when_each(yhas, lambda side: send_y(side, (FVY, FP, FVX, FD)))

    def not_(has):
        return lambda side: jnp.logical_not(has(side))

    def wall_y(side):
        for f in (FVZ, FVY, FVX, FD, FC):
            yrecv[side, f] = jnp.zeros((BX, BZ), jnp.float32)
        yrecv[side, FP] = V[PR, pl.ds(BY + face(side), BX, stride=BY), :]

    def wall_x(side):
        for f in (VX, VY, VZ):
            xrecv[side, f] = zero
        xrecv[side, PR] = V[PR, pl.ds(BY if side == 0 else ROWS, BY), :]
        FX[pl.ds(0 if side == 0 else ROWS + BY, BY), :] = zero

    when_each(not_(yhas), wall_y)
    when_each(not_(xhas), wall_x)

    when_each(xhas, lambda side: xcopy(1 - side).wait_recv())
    for side in range(2):
        sg = 0.5 if side == 0 else -0.5
        r = BY if side == 0 else ROWS
        g = G[pl.ds(r - BY, BY), :]
        coef = NU + sg * V[VX, pl.ds(r, BY), :]
        for k in range(3):
            n = coef * xrecv[side, k]
            if k == 0:
                n = n + sg * xrecv[side, PR]
            vel_o[k, pl.ds(r - BY, BY), :] += g * n

    for side in range(2):
        zcopy(1 - side, zsend, zrecv, zs, zr).wait_recv()
    for i in range(4):
        ln = pl.ds(BZ * i, BZ)
        vlo, vhi = zsend[0, 2:3, ln], zsend[1, 2:3, ln]
        clo, chi = NU + 0.5 * vlo, NU - 0.5 * vhi
        for k in range(3):
            nlo, nhi = clo * zrecv[0, k:k + 1, ln], chi * zrecv[1, k:k + 1, ln]
            if k == 2:
                nlo = nlo + 0.5 * zrecv[0, 3:4, ln]
                nhi = nhi - 0.5 * zrecv[1, 3:4, ln]
            Q[2 * k:2 * k + 1, ln] = nhi
            Q[2 * k + 1:2 * k + 2, ln] = nlo
        Q[6:7, ln] = zrecv[1, 4:5, ln]
        Q[7:8, ln] = zrecv[0, 4:5, ln]

    def unpack():
        for i in range(4):
            S[pl.ds(BZ * i, BZ), :] = Q[:, pl.ds(BZ * i, BZ)].T

    unpack()
    edge = (lane == 0) | (lane == BZ - 1)

    def zfix(x, carry):
        flow, void = carry
        o = pl.multiple_of(x * BY, BY)
        q, g, e = S[pl.ds(o, BY), :], G[pl.ds(o, BY), :], E[pl.ds(o, BY), :]
        for k in range(3):
            u = vel_o[k, pl.ds(o, BY), :] + g * jnp.where(edge, pltpu.roll(q, BZ - 1 - 2 * k, 1), 0.0)
            vel_o[k, pl.ds(o, BY), :] = u
        h = pltpu.roll(q, BZ - 7, 1)
        SL[pl.ds(o, BY), :] = 0.5 * (
            jnp.where(lane == BZ - 1, h, pltpu.roll(e, BZ - 1, 1))
            - jnp.where(lane == 0, h, pltpu.roll(e, 1, 1))
        )
        return flow + e * u, void + e

    flow, void = lax.fori_loop(0, BX, zfix, (zero, zero))

    def send_c(side):
        ycopy(side, FC).start()

    for side in range(2):
        ysend[side, FC] = (
            E[pl.ds(face(side), BX, stride=BY), :] * vel_o[VY, pl.ds(face(side), BX, stride=BY), :]
        )
    when_each(yhas, send_c)

    def ywait(side, fields):
        for f in fields:
            ycopy(1 - side, f).wait_recv()

    def yfix(side, k, f):
        sg = 0.5 if side == 0 else -0.5
        rows = pl.ds(face(side), BX, stride=BY)
        n = (NU + sg * ysend[side, FVY]) * yrecv[side, f]
        if k == VY:
            n = n + sg * yrecv[side, FP]
        g = G[rows, :]
        vel_o[k, rows, :] = vel_o[k, rows, :] + g * n
        return n

    when_each(yhas, lambda side: ywait(side, (FVZ,)))
    ysum = jnp.zeros((BX, BZ), jnp.float32)
    for side in range(2):
        ysum = ysum + ysend[side, FD] * yfix(side, VZ, FVZ)

    def spread(a, b):
        a, b = jnp.sum(a, axis=0, keepdims=True), jnp.sum(b, axis=0, keepdims=True)
        return jnp.where(
            lane[0:1] < BZ // 2, a + pltpu.roll(a, BZ // 2, 1), b + pltpu.roll(b, BZ // 2, 1)
        )

    part = spread(flow + (ysum[0:16] + ysum[16:32]), void)
    row1[0] = part
    red1[zabs] = part

    def c1(k):
        return remote(row1.at[0], red1.at[zabs], s1.at[k], r1.at[k], zpeers[k - 1])

    def c2(k):
        return remote(row2.at[0], red2.at[plane], s2.at[k], r2.at[k], ppeers[k - 1])

    for k in range(1, 16):
        c1(k).start()

    when_each(yhas, lambda side: ywait(side, (FVY, FP, FVX)))
    for side in range(2):
        yfix(side, VY, FVY)
        yfix(side, VX, FVX)

    def fluxes(x, carry):
        o = pl.multiple_of(x * BY, BY)
        e = E[pl.ds(o, BY), :]
        FX[pl.ds(o + BY, BY), :] = e * vel_o[VX, pl.ds(o, BY), :]
        fz = e * vel_o[VZ, pl.ds(o, BY), :]
        S[pl.ds(o, BY), :] = jnp.where(lane == 8, pltpu.roll(fz, 9, 1), fz)
        return carry

    lax.fori_loop(0, BX, fluxes, 0)
    for side in range(2):
        xsend2[side] = FX[pl.ds(BY if side == 0 else ROWS, BY), :]
    pack(zsend2)

    def xcopy2(side):
        return remote(
            xsend2.at[side], FX.at[pl.ds(ROWS + BY if side == 0 else 0, BY), :],
            xs2.at[side], xr2.at[1 - side], xlow if side == 0 else xhigh,
        )

    when_each(xhas, lambda side: xcopy2(side).start())
    for side in range(2):
        zcopy(side, zsend2, zrecv2, zs2, zr2).start()

    for k in range(1, 16):
        c1(k).wait_recv()
    part2 = red1[0]
    for i in range(1, 16):
        part2 = part2 + red1[i]
    row2[0] = part2
    red2[plane] = part2
    for k in range(1, 32):
        c2(k).start()

    when_each(yhas, lambda side: ywait(side, (FD, FC)))
    for side in range(2):
        sg = -0.5 if side == 0 else 0.5
        n = (NU + sg * yrecv[side, FVY]) * ysend[side, FVY] + sg * ysend[side, FP]
        yrecv[side, FC] = yrecv[side, FC] + yrecv[side, FD] * n

    for side in range(2):
        zcopy(1 - side, zsend2, zrecv2, zs2, zr2).wait_recv()
    Q[0:1, :] = zrecv2[1, 0:1, :]
    Q[1:2, :] = zrecv2[0, 0:1, :]
    unpack()
    when_each(xhas, lambda side: xcopy2(1 - side).wait_recv())

    def diverge(x, carry):
        o = pl.multiple_of(x * BY, BY)
        e = E[pl.ds(o, BY), :]
        fy = e * vel_o[VY, pl.ds(o, BY), :]
        fz = e * vel_o[VZ, pl.ds(o, BY), :]
        h = pltpu.roll(S[pl.ds(o, BY), :], BZ - 1, 1)
        d = FX[pl.ds(o + 2 * BY, BY), :] - FX[pl.ds(o, BY), :]
        d = d + (
            jnp.where(rown == BY - 1, yrecv[1, FC, pl.ds(x, 1), :], pltpu.roll(fy, BY - 1, 0))
            - jnp.where(rown == 0, yrecv[0, FC, pl.ds(x, 1), :], pltpu.roll(fy, 1, 0))
        )
        d = d + (
            jnp.where(lane == BZ - 1, h, pltpu.roll(fz, BZ - 1, 1))
            - jnp.where(lane == 0, h, pltpu.roll(fz, 1, 1))
        )
        src_o[pl.ds(o, BY), :] = 0.5 * d
        return carry

    lax.fori_loop(0, BX, diverge, 0)

    for k in range(1, 32):
        c2(k).wait_recv()
    total = red2[0]
    for i in range(1, 32):
        total = total + red2[i]
    half = lane[0:1] < BZ // 2
    flow_sum = jnp.sum(jnp.where(half, total, 0.0), axis=1, keepdims=True)
    void_sum = jnp.sum(jnp.where(half, 0.0, total), axis=1, keepdims=True)
    cells = float(ROWS * BZ * 512)
    step = (target_ref[0] * cells - flow_sum) / (DT * void_sum)
    force_o[...] = force + step
    add = jnp.broadcast_to(DT * step, (BY, BZ))

    def finish(x, carry):
        o = pl.multiple_of(x * BY, BY)
        vel_o[VZ, pl.ds(o, BY), :] += add
        src_o[pl.ds(o, BY), :] += add * SL[pl.ds(o, BY), :]
        return carry

    lax.fori_loop(0, BX, finish, 0)

    when_each(yhas, lambda side: [ycopy(side, f).wait_send() for f in range(6)] and None)
    when_each(xhas, lambda side: (xcopy(side).wait_send(), xcopy2(side).wait_send()) and None)
    for side in range(2):
        zcopy(side, zsend, zrecv, zs, zr).wait_send()
        zcopy(side, zsend2, zrecv2, zs2, zr2).wait_send()
    for k in range(1, 16):
        c1(k).wait_send()
    for k in range(1, 32):
        c2(k).wait_send()


def local(velocity, pressure, voidage, particle_vel, forcing, target_flux):
    f32 = jnp.float32
    vmem = pl.BlockSpec(memory_space=pltpu.VMEM)
    smem = pl.BlockSpec(memory_space=pltpu.SMEM)
    hbm = pl.BlockSpec(memory_space=pl.ANY)
    dma = pltpu.SemaphoreType.DMA
    vel, src, force = pl.pallas_call(
        kernel,
        out_shape=(
            jax.ShapeDtypeStruct((3, ROWS, BZ), f32),
            jax.ShapeDtypeStruct((ROWS, BZ), f32),
            jax.ShapeDtypeStruct((1, 1), f32),
        ),
        in_specs=[smem, smem, hbm, hbm, hbm, hbm],
        out_specs=(vmem, vmem, vmem),
        scratch_shapes=[
            pltpu.VMEM((4, PAD, BZ), f32),
            pltpu.VMEM((ROWS, BZ), f32),
            pltpu.VMEM((3, ROWS, BZ), f32),
            pltpu.VMEM((ROWS, BZ), f32),
            pltpu.VMEM((ROWS, BZ), f32),
            pltpu.VMEM((ROWS, BZ), f32),
            pltpu.VMEM((PAD, BZ), f32),
            pltpu.VMEM((BZ, ROWS), f32),
            pltpu.VMEM((2, 4, BY, BZ), f32),
            pltpu.VMEM((2, 8, ROWS), f32),
            pltpu.VMEM((2, 8, ROWS), f32),
            pltpu.VMEM((2, 8, ROWS), f32),
            pltpu.VMEM((2, 8, ROWS), f32),
            pltpu.VMEM((2, 6, BX, BZ), f32),
            pltpu.VMEM((2, 6, BX, BZ), f32),
            pltpu.VMEM((2, BY, BZ), f32),
            pltpu.VMEM((1, 1, BZ), f32),
            pltpu.VMEM((16, 1, BZ), f32),
            pltpu.VMEM((1, 1, BZ), f32),
            pltpu.VMEM((32, 1, BZ), f32),
            dma((4,)), dma((2,)), dma((2,)), dma((2,)), dma((2,)), dma((2,)), dma((2,)),
            dma((2, 6)), dma((2, 6)), dma((2,)), dma((2,)),
            dma((16,)), dma((16,)), dma((32,)), dma((32,)),
        ],
        compiler_params=pltpu.CompilerParams(collective_id=0, has_side_effects=True),
    )(
        forcing,
        target_flux,
        velocity.reshape(3, ROWS, BZ),
        pressure.reshape(ROWS, BZ),
        voidage.reshape(ROWS, BZ),
        particle_vel.reshape(3, ROWS, BZ),
    )
    return vel.reshape(3, BX, BY, BZ), src.reshape(BX, BY, BZ), force.reshape(1)


def solution(mesh):
    return jax.shard_map(
        local,
        mesh=mesh,
        in_specs=(
            P(None, "gx", "gy", "gz"), P("gx", "gy", "gz"), P("gx", "gy", "gz"),
            P(None, "gx", "gy", "gz"), P(), P(),
        ),
        out_specs=(P(None, "gx", "gy", "gz"), P("gx", "gy", "gz"), P()),
        check_vma=False,
    )
```

```python
import jax
import jax.numpy as jnp
from jax import lax
from jax.experimental import pallas as pl
from jax.experimental.pallas import tpu as pltpu
from jax.sharding import PartitionSpec as P

MESH = pl.DeviceIdType.MESH
DT = 0.2
NU = 0.1
BX, BY, BZ = 32, 16, 128
ROWS = BX * BY
PAD = ROWS + 2 * BY
VX, VY, VZ, PR = 0, 1, 2, 3
FVZ, FVY, FP, FVX, FD, FC = 0, 1, 2, 3, 4, 5


def kernel(
    force_h, target_h, vel_h, pres_h, eps_h, pv_h,
    vel_o, src_o, SL, aux_o,
    V, E, PV, G, S, FX, Q, scal,
    xrecv, zsend, zrecv, zsend2, zrecv2, ysend, yrecv, xsend2,
    row1, red1, row2, red2,
    lsem, xs, xr, zs, zr, zs2, zr2, ys, yr, xs2, xr2, s1, r1, s2, r2,
):
    gz, gy, gx = lax.axis_index("gz"), lax.axis_index("gy"), lax.axis_index("gx")
    ngz, ngy, ngx = 16, 8, 4
    here = {"gz": gz, "gy": gy, "gx": gx}

    def at(**kw):
        return {**here, **kw}

    y, zhi = gy // 2, gy % 2
    zlo, core = gz // 2, gz % 2
    zabs = zhi * 8 + zlo
    xi, yi = gx, y
    has_xlo, has_xhi = gx > 0, gx < ngx - 1
    has_ylo, has_yhi = gy > 0, gy < ngy - 1

    def of_z(z):
        return at(gz=lax.rem(z, 8) * 2 + core, gy=y * 2 + z // 8)

    def of_plane(i):
        return at(gx=i // 8, gy=lax.rem(i // 2, 4) * 2 + zhi, gz=zlo * 2 + lax.rem(i, 2))

    plane = gx * 8 + y * 2 + core
    zpeers = [of_z(lax.rem(zabs + k, 16)) for k in range(1, 16)]
    ppeers = [of_plane(lax.rem(plane + k, 32)) for k in range(1, 32)]
    zlow, zhigh = at(gz=lax.rem(gz + ngz - 1, ngz)), at(gz=lax.rem(gz + 1, ngz))
    ylow, yhigh = at(gy=lax.rem(gy + ngy - 1, ngy)), at(gy=lax.rem(gy + 1, ngy))
    xlow, xhigh = at(gx=lax.rem(gx + ngx - 1, ngx)), at(gx=lax.rem(gx + 1, ngx))

    barrier = pltpu.get_barrier_semaphore()
    partners = [ylow, yhigh] + zpeers + [zlow, zhigh] + ppeers
    for d in partners:
        pl.semaphore_signal(barrier, inc=1, device_id=d, device_id_type=MESH)

    loads = [
        pltpu.make_async_copy(vel_h, V.at[pl.ds(0, 3), pl.ds(BY, ROWS), :], lsem.at[0]),
        pltpu.make_async_copy(pres_h, V.at[3, pl.ds(BY, ROWS), :], lsem.at[1]),
        pltpu.make_async_copy(eps_h, E, lsem.at[2]),
        pltpu.make_async_copy(pv_h, PV, lsem.at[3]),
        pltpu.make_async_copy(force_h, scal.at[0], lsem.at[4]),
        pltpu.make_async_copy(target_h, scal.at[1], lsem.at[5]),
    ]
    for cp in loads:
        cp.start()

    lane = lax.broadcasted_iota(jnp.int32, (BY, BZ), 1)
    rown = lax.broadcasted_iota(jnp.int32, (BY, BZ), 0)
    zero = jnp.zeros((BY, BZ), jnp.float32)
    for f in range(4):
        V[f, pl.ds(0, BY), :] = zero
        V[f, pl.ds(ROWS + BY, BY), :] = zero
    Q[...] = jnp.zeros_like(Q)
    for cp in loads:
        cp.wait()
    force, target = scal[0, 0], scal[1, 0]

    def face(side):
        return 0 if side == 0 else BY - 1

    for side in range(2):
        for slot, f in ((FVZ, VZ), (FVY, VY), (FP, PR), (FVX, VX)):
            ysend[side, slot] = V[f, pl.ds(BY + face(side), BX, stride=BY), :]

    def slab(x, carry):
        o = pl.multiple_of(x * BY, BY)
        c = [V[f, pl.ds(o + BY, BY), :] for f in range(4)]
        xm = [V[f, pl.ds(o, BY), :] for f in range(4)]
        xp = [V[f, pl.ds(o + 2 * BY, BY), :] for f in range(4)]
        e = E[pl.ds(o, BY), :]
        pv = [PV[k, pl.ds(o, BY), :] for k in range(3)]
        zm = [jnp.where(lane == 0, 0.0, pltpu.roll(a, 1, 1)) for a in c]
        zp = [jnp.where(lane == BZ - 1, 0.0, pltpu.roll(a, BZ - 1, 1)) for a in c]
        ym = [jnp.where(rown == 0, 0.0, pltpu.roll(a, 1, 0)) for a in c]
        yp = [jnp.where(rown == BY - 1, 0.0, pltpu.roll(a, BY - 1, 0)) for a in c]
        slip = jnp.sqrt(
            (c[0] - pv[0]) * (c[0] - pv[0])
            + (c[1] - pv[1]) * (c[1] - pv[1])
            + (c[2] - pv[2]) * (c[2] - pv[2])
        )
        drag = (1.0 - e) * jnp.exp(-2.65 * jnp.log(e)) * (1.0 + slip)
        w = 1.0 / (1.0 + DT * drag)
        hi, lo = (xp, yp, zp), (xm, ym, zm)
        for k in range(3):
            adv = zero
            lap = -6.0 * c[k]
            for d in range(3):
                adv = adv + c[d] * (hi[d][k] - lo[d][k])
                lap = lap + hi[d][k] + lo[d][k]
            fk = NU * lap - 0.5 * (adv + (hi[k][3] - lo[k][3]))
            if k == 2:
                fk = fk + force
            vel_o[k, pl.ds(o, BY), :] = (c[k] + DT * (fk + drag * pv[k])) * w
        G[pl.ds(o, BY), :] = DT * w
        s = zero
        for k, a in enumerate(c + [e]):
            s = jnp.where(lane == k, a if k == 0 else pltpu.roll(a, k, 1), s)
            s = jnp.where(lane == 8 + k, pltpu.roll(a, 9 + k, 1), s)
        S[pl.ds(o, BY), :] = s
        return carry

    lax.fori_loop(0, BX, slab, 0)

    def pack(dst):
        for i in range(4):
            t = S[pl.ds(BZ * i, BZ), :].T
            dst[0, :, pl.ds(BZ * i, BZ)] = t[0:8]
            dst[1, :, pl.ds(BZ * i, BZ)] = t[8:16]

    pack(zsend)
    for side in range(2):
        ysend[side, FD] = (
            E[pl.ds(face(side), BX, stride=BY), :] * G[pl.ds(face(side), BX, stride=BY), :]
        )

    pl.semaphore_wait(barrier, len(partners))

    def remote(src, dst, a, b, dev):
        return pltpu.make_async_remote_copy(
            src_ref=src, dst_ref=dst, send_sem=a, recv_sem=b, device_id=dev, device_id_type=MESH
        )

    def ycopy(side, f):
        return remote(
            ysend.at[side, f], yrecv.at[1 - side, f], ys.at[side, f], yr.at[1 - side, f],
            ylow if side == 0 else yhigh,
        )

    def yhas(side):
        return has_ylo if side == 0 else has_yhi

    def xcopy(side):
        r = BY if side == 0 else ROWS
        return remote(
            V.at[:, pl.ds(r, BY), :], xrecv.at[1 - side], xs.at[side], xr.at[1 - side],
            xlow if side == 0 else xhigh,
        )

    def xhas(side):
        return has_xlo if side == 0 else has_xhi

    def zcopy(side, src, dst, a, b):
        return remote(
            src.at[side], dst.at[1 - side], a.at[side], b.at[1 - side],
            zlow if side == 0 else zhigh,
        )

    def when_each(has, fn):
        for side in range(2):
            pl.when(has(side))(lambda side=side: fn(side))

    def send_y(side, fields):
        for f in fields:
            ycopy(side, f).start()

    when_each(yhas, lambda side: send_y(side, (FVZ,)))
    for side in range(2):
        zcopy(side, zsend, zrecv, zs, zr).start()
    when_each(xhas, lambda side: xcopy(side).start())
    when_each(yhas, lambda side: send_y(side, (FVY, FP, FVX, FD)))

    def not_(has):
        return lambda side: jnp.logical_not(has(side))

    def wall_y(side):
        for f in (FVZ, FVY, FVX, FD, FC):
            yrecv[side, f] = jnp.zeros((BX, BZ), jnp.float32)
        yrecv[side, FP] = V[PR, pl.ds(BY + face(side), BX, stride=BY), :]

    def wall_x(side):
        for f in (VX, VY, VZ):
            xrecv[side, f] = zero
        xrecv[side, PR] = V[PR, pl.ds(BY if side == 0 else ROWS, BY), :]
        FX[pl.ds(0 if side == 0 else ROWS + BY, BY), :] = zero

    when_each(not_(yhas), wall_y)
    when_each(not_(xhas), wall_x)

    when_each(xhas, lambda side: xcopy(1 - side).wait_recv())
    for side in range(2):
        sg = 0.5 if side == 0 else -0.5
        r = BY if side == 0 else ROWS
        g = G[pl.ds(r - BY, BY), :]
        coef = NU + sg * V[VX, pl.ds(r, BY), :]
        for k in range(3):
            n = coef * xrecv[side, k]
            if k == 0:
                n = n + sg * xrecv[side, PR]
            vel_o[k, pl.ds(r - BY, BY), :] += g * n

    for side in range(2):
        zcopy(1 - side, zsend, zrecv, zs, zr).wait_recv()
    for i in range(4):
        ln = pl.ds(BZ * i, BZ)
        vlo, vhi = zsend[0, 2:3, ln], zsend[1, 2:3, ln]
        clo, chi = NU + 0.5 * vlo, NU - 0.5 * vhi
        for k in range(3):
            nlo, nhi = clo * zrecv[0, k:k + 1, ln], chi * zrecv[1, k:k + 1, ln]
            if k == 2:
                nlo = nlo + 0.5 * zrecv[0, 3:4, ln]
                nhi = nhi - 0.5 * zrecv[1, 3:4, ln]
            Q[2 * k:2 * k + 1, ln] = nhi
            Q[2 * k + 1:2 * k + 2, ln] = nlo
        Q[6:7, ln] = zrecv[1, 4:5, ln]
        Q[7:8, ln] = zrecv[0, 4:5, ln]

    def unpack():
        for i in range(4):
            S[pl.ds(BZ * i, BZ), :] = Q[:, pl.ds(BZ * i, BZ)].T

    unpack()
    edge = (lane == 0) | (lane == BZ - 1)

    def zfix(x, carry):
        flow, void = carry
        o = pl.multiple_of(x * BY, BY)
        q, g, e = S[pl.ds(o, BY), :], G[pl.ds(o, BY), :], E[pl.ds(o, BY), :]
        for k in range(3):
            u = vel_o[k, pl.ds(o, BY), :] + g * jnp.where(edge, pltpu.roll(q, BZ - 1 - 2 * k, 1), 0.0)
            vel_o[k, pl.ds(o, BY), :] = u
        h = pltpu.roll(q, BZ - 7, 1)
        SL[pl.ds(o, BY), :] = 0.5 * (
            jnp.where(lane == BZ - 1, h, pltpu.roll(e, BZ - 1, 1))
            - jnp.where(lane == 0, h, pltpu.roll(e, 1, 1))
        )
        return flow + e * u, void + e

    flow, void = lax.fori_loop(0, BX, zfix, (zero, zero))

    def send_c(side):
        ycopy(side, FC).start()

    for side in range(2):
        ysend[side, FC] = (
            E[pl.ds(face(side), BX, stride=BY), :] * vel_o[VY, pl.ds(face(side), BX, stride=BY), :]
        )
    when_each(yhas, send_c)

    def ywait(side, fields):
        for f in fields:
            ycopy(1 - side, f).wait_recv()

    def yfix(side, k, f):
        sg = 0.5 if side == 0 else -0.5
        rows = pl.ds(face(side), BX, stride=BY)
        n = (NU + sg * ysend[side, FVY]) * yrecv[side, f]
        if k == VY:
            n = n + sg * yrecv[side, FP]
        g = G[rows, :]
        vel_o[k, rows, :] = vel_o[k, rows, :] + g * n
        return n

    when_each(yhas, lambda side: ywait(side, (FVZ,)))
    ysum = jnp.zeros((BX, BZ), jnp.float32)
    for side in range(2):
        ysum = ysum + ysend[side, FD] * yfix(side, VZ, FVZ)

    def spread(a, b):
        a, b = jnp.sum(a, axis=0, keepdims=True), jnp.sum(b, axis=0, keepdims=True)
        return jnp.where(
            lane[0:1] < BZ // 2, a + pltpu.roll(a, BZ // 2, 1), b + pltpu.roll(b, BZ // 2, 1)
        )

    part = spread(flow + (ysum[0:16] + ysum[16:32]), void)
    row1[0] = part
    red1[zabs] = part

    def c1(k):
        return remote(row1.at[0], red1.at[zabs], s1.at[k], r1.at[k], zpeers[k - 1])

    def c2(k):
        return remote(row2.at[0], red2.at[plane], s2.at[k], r2.at[k], ppeers[k - 1])

    for k in range(1, 16):
        c1(k).start()

    when_each(yhas, lambda side: ywait(side, (FVY, FP, FVX)))
    for side in range(2):
        yfix(side, VY, FVY)
        yfix(side, VX, FVX)

    def fluxes(x, carry):
        o = pl.multiple_of(x * BY, BY)
        e = E[pl.ds(o, BY), :]
        FX[pl.ds(o + BY, BY), :] = e * vel_o[VX, pl.ds(o, BY), :]
        fz = e * vel_o[VZ, pl.ds(o, BY), :]
        S[pl.ds(o, BY), :] = jnp.where(lane == 8, pltpu.roll(fz, 9, 1), fz)
        return carry

    lax.fori_loop(0, BX, fluxes, 0)
    for side in range(2):
        xsend2[side] = FX[pl.ds(BY if side == 0 else ROWS, BY), :]
    pack(zsend2)

    def xcopy2(side):
        return remote(
            xsend2.at[side], FX.at[pl.ds(ROWS + BY if side == 0 else 0, BY), :],
            xs2.at[side], xr2.at[1 - side], xlow if side == 0 else xhigh,
        )

    when_each(xhas, lambda side: xcopy2(side).start())
    for side in range(2):
        zcopy(side, zsend2, zrecv2, zs2, zr2).start()

    for k in range(1, 16):
        c1(k).wait_recv()
    part2 = red1[0]
    for i in range(1, 16):
        part2 = part2 + red1[i]
    row2[0] = part2
    red2[plane] = part2
    for k in range(1, 32):
        c2(k).start()

    when_each(yhas, lambda side: ywait(side, (FD, FC)))
    for side in range(2):
        sg = -0.5 if side == 0 else 0.5
        n = (NU + sg * yrecv[side, FVY]) * ysend[side, FVY] + sg * ysend[side, FP]
        yrecv[side, FC] = yrecv[side, FC] + yrecv[side, FD] * n

    for side in range(2):
        zcopy(1 - side, zsend2, zrecv2, zs2, zr2).wait_recv()
    Q[0:1, :] = zrecv2[1, 0:1, :]
    Q[1:2, :] = zrecv2[0, 0:1, :]
    unpack()
    when_each(xhas, lambda side: xcopy2(1 - side).wait_recv())

    def diverge(x, carry):
        o = pl.multiple_of(x * BY, BY)
        e = E[pl.ds(o, BY), :]
        fy = e * vel_o[VY, pl.ds(o, BY), :]
        fz = e * vel_o[VZ, pl.ds(o, BY), :]
        h = pltpu.roll(S[pl.ds(o, BY), :], BZ - 1, 1)
        d = FX[pl.ds(o + 2 * BY, BY), :] - FX[pl.ds(o, BY), :]
        d = d + (
            jnp.where(rown == BY - 1, yrecv[1, FC, pl.ds(x, 1), :], pltpu.roll(fy, BY - 1, 0))
            - jnp.where(rown == 0, yrecv[0, FC, pl.ds(x, 1), :], pltpu.roll(fy, 1, 0))
        )
        d = d + (
            jnp.where(lane == BZ - 1, h, pltpu.roll(fz, BZ - 1, 1))
            - jnp.where(lane == 0, h, pltpu.roll(fz, 1, 1))
        )
        src_o[pl.ds(o, BY), :] = 0.5 * d
        return carry

    lax.fori_loop(0, BX, diverge, 0)

    for k in range(1, 32):
        c2(k).wait_recv()
    total = red2[0]
    for i in range(1, 32):
        total = total + red2[i]
    half = lane[0:1] < BZ // 2
    flow_sum = jnp.sum(jnp.where(half, total, 0.0), axis=1, keepdims=True)
    void_sum = jnp.sum(jnp.where(half, 0.0, total), axis=1, keepdims=True)
    cells = float(ROWS * BZ * 512)
    step = (target * cells - flow_sum) / (DT * void_sum)
    aux_o[0:1, :] = jnp.broadcast_to(DT * step, (1, BZ))
    aux_o[1:2, :] = jnp.broadcast_to(force + step, (1, BZ))

    when_each(yhas, lambda side: [ycopy(side, f).wait_send() for f in range(6)] and None)
    when_each(xhas, lambda side: (xcopy(side).wait_send(), xcopy2(side).wait_send()) and None)
    for side in range(2):
        zcopy(side, zsend, zrecv, zs, zr).wait_send()
        zcopy(side, zsend2, zrecv2, zs2, zr2).wait_send()
    for k in range(1, 16):
        c1(k).wait_send()
    for k in range(1, 32):
        c2(k).wait_send()


def finish(vel, src, slope, aux, vel_o, src_o, force_o, vz, out, sem):
    pairs = [
        pltpu.make_async_copy(vel.at[pl.ds(0, 2)], vel_o.at[pl.ds(0, 2)], sem.at[0]),
        pltpu.make_async_copy(vz, vel_o.at[VZ], sem.at[1]),
        pltpu.make_async_copy(out, src_o, sem.at[2]),
    ]
    pairs[0].start()
    force_o[...] = aux[1:2, 0:1]
    add = aux[0:1, :]
    vz[...] = vel[VZ] + add
    pairs[1].start()
    out[...] = src[...] + add * slope[...]
    pairs[2].start()
    for cp in pairs:
        cp.wait()


def local(velocity, pressure, voidage, particle_vel, forcing, target_flux):
    f32 = jnp.float32
    vmem = pl.BlockSpec(memory_space=pltpu.VMEM)
    hbm = pl.BlockSpec(memory_space=pl.ANY)
    dma = pltpu.SemaphoreType.DMA
    parts = pl.pallas_call(
        kernel,
        out_shape=(
            pltpu.VMEM((3, ROWS, BZ), f32),
            pltpu.VMEM((ROWS, BZ), f32),
            pltpu.VMEM((ROWS, BZ), f32),
            pltpu.VMEM((8, BZ), f32),
        ),
        in_specs=[pl.BlockSpec(memory_space=pltpu.HBM)] * 6,
        out_specs=(vmem,) * 4,
        scratch_shapes=[
            pltpu.VMEM((4, PAD, BZ), f32),
            pltpu.VMEM((ROWS, BZ), f32),
            pltpu.VMEM((3, ROWS, BZ), f32),
            pltpu.VMEM((ROWS, BZ), f32),
            pltpu.VMEM((ROWS, BZ), f32),
            pltpu.VMEM((PAD, BZ), f32),
            pltpu.VMEM((BZ, ROWS), f32),
            pltpu.SMEM((2, 1), f32),
            pltpu.VMEM((2, 4, BY, BZ), f32),
            pltpu.VMEM((2, 8, ROWS), f32),
            pltpu.VMEM((2, 8, ROWS), f32),
            pltpu.VMEM((2, 8, ROWS), f32),
            pltpu.VMEM((2, 8, ROWS), f32),
            pltpu.VMEM((2, 6, BX, BZ), f32),
            pltpu.VMEM((2, 6, BX, BZ), f32),
            pltpu.VMEM((2, BY, BZ), f32),
            pltpu.VMEM((1, 1, BZ), f32),
            pltpu.VMEM((16, 1, BZ), f32),
            pltpu.VMEM((1, 1, BZ), f32),
            pltpu.VMEM((32, 1, BZ), f32),
            dma((6,)), dma((2,)), dma((2,)), dma((2,)), dma((2,)), dma((2,)), dma((2,)),
            dma((2, 6)), dma((2, 6)), dma((2,)), dma((2,)),
            dma((16,)), dma((16,)), dma((32,)), dma((32,)),
        ],
        compiler_params=pltpu.CompilerParams(collective_id=0, has_side_effects=True),
    )(
        forcing,
        target_flux,
        velocity.reshape(3, ROWS, BZ),
        pressure.reshape(ROWS, BZ),
        voidage.reshape(ROWS, BZ),
        particle_vel.reshape(3, ROWS, BZ),
    )
    vel, src, force = pl.pallas_call(
        finish,
        out_shape=(
            jax.ShapeDtypeStruct((3, ROWS, BZ), f32),
            jax.ShapeDtypeStruct((ROWS, BZ), f32),
            jax.ShapeDtypeStruct((1, 1), f32),
        ),
        in_specs=[vmem] * 4,
        out_specs=(hbm, hbm, vmem),
        scratch_shapes=[pltpu.VMEM((ROWS, BZ), f32), pltpu.VMEM((ROWS, BZ), f32), dma((3,))],
        compiler_params=pltpu.CompilerParams(vmem_limit_bytes=8 * 1024 * 1024),
    )(*[pltpu.with_memory_space_constraint(p, pltpu.VMEM) for p in parts])
    return vel.reshape(3, BX, BY, BZ), src.reshape(BX, BY, BZ), force.reshape(1)


def solution(mesh):
    return jax.shard_map(
        local,
        mesh=mesh,
        in_specs=(
            P(None, "gx", "gy", "gz"), P("gx", "gy", "gz"), P("gx", "gy", "gz"),
            P(None, "gx", "gy", "gz"), P(), P(),
        ),
        out_specs=(P(None, "gx", "gy", "gz"), P("gx", "gy", "gz"), P()),
        check_vma=False,
    )
```

```python
import jax
import jax.numpy as jnp
from jax import lax
from jax.experimental import pallas as pl
from jax.experimental.pallas import tpu as pltpu
from jax.sharding import PartitionSpec as P

MESH = pl.DeviceIdType.MESH
DT = 0.2
NU = 0.1
BX, BY, BZ = 32, 16, 128
ROWS = BX * BY
PAD = ROWS + 2 * BY
VX, VY, VZ, PR = 0, 1, 2, 3
FVZ, FVY, FD, FP, FVX, FC = 0, 1, 2, 3, 4, 5
GROUPS = ((0, 3), (3, 2), (5, 1))
NZ_, NY_, NX_, NF_ = 0, 1, 2, 3
BACK = ((0, 1), (1, 2), (3, 1))


def weight(c, pv, e):
    a, b, d = c[0] - pv[0], c[1] - pv[1], c[2] - pv[2]
    slip = jnp.sqrt(a * a + b * b + d * d)
    drag = (1.0 - e) * jnp.exp(-2.65 * jnp.log(e)) * (1.0 + slip)
    return drag, 1.0 / (1.0 + DT * drag)


def kernel(
    force_h, target_h, vel_h, pres_h, eps_h, pv_h,
    vel_o, src_o, SL, aux_o,
    V, E, PV, G, S, FX, Q, scal,
    xrecv, zsend, zrecv, zsend2, zrecv2, ysend, yrecv, msend, mrecv, yacc, xsend2, rbuf,
    row1, red1, row2, red2,
    lsem, xs, xr, zs, zr, zs2, zr2, ys, yr, ms, mr, xs2, xr2, s1, r1, s2, r2, know, wave, cross, rsem, fsem,
):
    gz, gy, gx = lax.axis_index("gz"), lax.axis_index("gy"), lax.axis_index("gx")
    ngz, ngy, ngx = 16, 8, 4
    here = {"gz": gz, "gy": gy, "gx": gx}

    def at(**kw):
        return {**here, **kw}

    y, zhi = gy // 2, gy % 2
    zlo, core = gz // 2, gz % 2
    zabs = zhi * 8 + zlo
    xi, yi = gx, y
    has_xlo, has_xhi = gx > 0, gx < ngx - 1
    has_ylo, has_yhi = gy > 0, gy < ngy - 1

    def of_z(z, dy=0):
        z, yy = lax.rem(z, 16), lax.rem(y + dy + 4, 4)
        return at(gz=lax.rem(z, 8) * 2 + core, gy=yy * 2 + z // 8)

    def of_plane(i):
        return at(gx=i // 8, gy=lax.rem(i // 2, 4) * 2 + zhi, gz=zlo * 2 + lax.rem(i, 2))

    plane = gx * 8 + y * 2 + core
    zpeers = [of_z(zabs + k) for k in range(1, 16)]
    ppeers = [of_plane(lax.rem(plane + k, 32)) for k in range(1, 32)]
    zlow, zhigh = at(gz=lax.rem(gz + ngz - 1, ngz)), at(gz=lax.rem(gz + 1, ngz))
    xlow, xhigh = at(gx=lax.rem(gx + ngx - 1, ngx)), at(gx=lax.rem(gx + 1, ngx))

    barrier = pltpu.get_barrier_semaphore()
    below, above = [of_z(zabs + 16 - k) for k in (1, 2, 4)], [of_z(zabs + k) for k in (1, 2, 4)]
    yprev, ynext = of_z(zabs, -1), of_z(zabs, 1)
    other = at(gz=zlo * 2 + 1 - core)
    outer_far = (gz == 0) | (gz == ngz - 1)
    outer = at(gz=lax.rem(gz + ngz - 1 + 2 * core, ngz))
    nearest = [below[0], above[0], other, xlow, xhigh, yprev, ynext]
    for d in nearest:
        pl.semaphore_signal(barrier, inc=1, device_id=d, device_id_type=MESH)

    @pl.when(jnp.logical_not(outer_far))
    def _():
        pl.semaphore_signal(barrier, inc=1, device_id=outer, device_id_type=MESH)

    loads = [
        pltpu.make_async_copy(vel_h, V.at[pl.ds(0, 3), pl.ds(BY, ROWS), :], lsem.at[0]),
        pltpu.make_async_copy(pres_h, V.at[3, pl.ds(BY, ROWS), :], lsem.at[1]),
        pltpu.make_async_copy(eps_h, E, lsem.at[2]),
        pltpu.make_async_copy(pv_h, PV, lsem.at[3]),
        pltpu.make_async_copy(force_h, scal.at[0], lsem.at[4]),
        pltpu.make_async_copy(target_h, scal.at[1], lsem.at[5]),
    ]
    for cp in loads:
        cp.start()

    lane = lax.broadcasted_iota(jnp.int32, (BY, BZ), 1)
    rown = lax.broadcasted_iota(jnp.int32, (BY, BZ), 0)
    zero = jnp.zeros((BY, BZ), jnp.float32)
    for f in range(4):
        V[f, pl.ds(0, BY), :] = zero
        V[f, pl.ds(ROWS + BY, BY), :] = zero
    Q[...] = jnp.zeros_like(Q)
    def tell(step):
        pl.semaphore_signal(know.at[step, 0], inc=1, device_id=above[step], device_id_type=MESH)
        pl.semaphore_signal(know.at[step, 1], inc=1, device_id=below[step], device_id_type=MESH)

    def heard(step, side):
        pl.semaphore_wait(know.at[step, side], 1)

    waves = [(xlow, xhigh), (yprev, ynext), (yprev, ynext), (other,)]

    def plane_tell(i):
        for d in waves[i]:
            pl.semaphore_signal(wave.at[i], inc=1, device_id=d, device_id_type=MESH)

    def plane_heard(i):
        pl.semaphore_wait(wave.at[i], len(waves[i]))

    pl.semaphore_wait(barrier, len(nearest) + jnp.where(outer_far, 0, 1))
    tell(0)
    plane_tell(0)

    for cp in loads:
        cp.wait()
    force, target = scal[0, 0], scal[1, 0]

    def face(side):
        return 0 if side == 0 else BY - 1

    for side in range(2):
        rows = pl.ds(face(side), BX, stride=BY)
        v = [V[f, pl.ds(BY + face(side), BX, stride=BY), :] for f in range(4)]
        ysend[side, FVZ], ysend[side, FVY] = v[VZ], v[VY]
        ysend[side, FP], ysend[side, FVX] = v[PR], v[VX]
        e = E[rows, :]
        ysend[side, FD] = e * DT * weight(v, [PV[k, rows, :] for k in range(3)], e)[1]

    heard(0, 0)
    heard(0, 1)
    tell(1)

    def remote(src, dst, a, b, dev):
        return pltpu.make_async_remote_copy(
            src_ref=src, dst_ref=dst, send_sem=a, recv_sem=b, device_id=dev, device_id_type=MESH
        )

    def side_of(kind):
        return 1 - zhi if kind == 0 else zhi

    def ycopy(kind, j):
        side, part = side_of(kind), pl.ds(*GROUPS[j])
        return remote(
            ysend.at[side, part], mrecv.at[1 - side, part], ys.at[kind, j], mr.at[1 - side, j],
            of_z(zabs + 12 + 8 * side, kind * zhi),
        )

    def paired(kind):
        return (gy >= 0) if kind == 0 else jnp.where(zhi == 0, y, 3 - y) > 0

    def mwait(q, j):
        part = pl.ds(*GROUPS[j])
        remote(ysend.at[0, part], mrecv.at[q, part], ys.at[0, j], mr.at[q, j], above[2]).wait_recv()

    def yhas(side):
        return has_ylo if side == 0 else has_yhi

    intra = (zabs >= 4) & (zabs < 12)
    middle = intra | (y > 0)

    def mcopy(q, j):
        part = pl.ds(*BACK[j])
        return remote(
            msend.at[q, part], yrecv.at[1 - q, part], ms.at[q, j], yr.at[1 - q, j],
            of_z(zabs + 12, jnp.where(intra, 0, -1)) if q == 0 else of_z(zabs + 4),
        )

    def xcopy(side):
        r = BY if side == 0 else ROWS
        return remote(
            V.at[:, pl.ds(r, BY), :], xrecv.at[1 - side], xs.at[side], xr.at[1 - side],
            xlow if side == 0 else xhigh,
        )

    def xhas(side):
        return has_xlo if side == 0 else has_xhi

    def zcopy(side, src, dst, a, b):
        return remote(
            src.at[side], dst.at[1 - side], a.at[side], b.at[1 - side],
            zlow if side == 0 else zhigh,
        )

    def when_each(has, fn):
        for side in range(2):
            pl.when(has(side))(lambda side=side: fn(side))

    def send_y(kind, groups):
        @pl.when(paired(kind))
        def _():
            for g in groups:
                ycopy(kind, g).start()

    when_each(xhas, lambda side: xcopy(side).start())
    plane_heard(0)
    plane_tell(1)

    def columns(x, carry):
        o = pl.multiple_of(x * BY, BY)
        s = zero
        for k, a in enumerate([V[f, pl.ds(o + BY, BY), :] for f in range(4)] + [E[pl.ds(o, BY), :]]):
            s = jnp.where(lane == k, a if k == 0 else pltpu.roll(a, k, 1), s)
            s = jnp.where(lane == 8 + k, pltpu.roll(a, 9 + k, 1), s)
        S[pl.ds(o, BY), :] = s
        return carry

    lax.fori_loop(0, BX, columns, 0, unroll=4)

    def pack(dst):
        for i in range(4):
            t = S[pl.ds(BZ * i, BZ), :].T
            dst[0, :, pl.ds(BZ * i, BZ)] = t[0:8]
            dst[1, :, pl.ds(BZ * i, BZ)] = t[8:16]

    pack(zsend)
    relay = zlo == 4 - core

    def zwrap():
        return remote(
            zsend.at[core], rbuf, zs.at[core], rsem, of_z(zabs + 20 - 8 * core),
        )

    def zforward():
        return remote(
            rbuf, zrecv.at[1 - core], fsem, zr.at[1 - core], at(gz=gz + 7 - 14 * core),
        )

    for side in range(2):
        @pl.when(jnp.logical_not(outer_far & (core == side)))
        def _():
            zcopy(side, zsend, zrecv, zs, zr).start()

    heard(1, 1 - zhi)
    send_y(0, (0,))
    heard(1, zhi)

    tell(2)

    @pl.when(outer_far)
    def _():
        zwrap().start()

    @pl.when(zhi == 1)
    def _():
        pl.semaphore_signal(
            cross, inc=1, device_id=of_z(zabs, -1), device_id_type=MESH
        )
        pl.semaphore_wait(cross, 1)

    send_y(1, (0,))

    plane_heard(1)
    plane_tell(2)

    def slab(x, carry):
        o = pl.multiple_of(x * BY, BY)
        c = [V[f, pl.ds(o + BY, BY), :] for f in range(4)]
        xm = [V[f, pl.ds(o, BY), :] for f in range(4)]
        xp = [V[f, pl.ds(o + 2 * BY, BY), :] for f in range(4)]
        e = E[pl.ds(o, BY), :]
        pv = [PV[k, pl.ds(o, BY), :] for k in range(3)]
        zm = [jnp.where(lane == 0, 0.0, pltpu.roll(a, 1, 1)) for a in c]
        zp = [jnp.where(lane == BZ - 1, 0.0, pltpu.roll(a, BZ - 1, 1)) for a in c]
        ym = [jnp.where(rown == 0, 0.0, pltpu.roll(a, 1, 0)) for a in c]
        yp = [jnp.where(rown == BY - 1, 0.0, pltpu.roll(a, BY - 1, 0)) for a in c]
        drag, w = weight(c, pv, e)
        hi, lo = (xp, yp, zp), (xm, ym, zm)
        for k in range(3):
            adv = zero
            lap = -6.0 * c[k]
            for d in range(3):
                adv = adv + c[d] * (hi[d][k] - lo[d][k])
                lap = lap + hi[d][k] + lo[d][k]
            fk = NU * lap - 0.5 * (adv + (hi[k][3] - lo[k][3]))
            if k == 2:
                fk = fk + force
            vel_o[k, pl.ds(o, BY), :] = (c[k] + DT * (fk + drag * pv[k])) * w
        G[pl.ds(o, BY), :] = DT * w
        return carry

    lax.fori_loop(0, BX, slab, 0, unroll=4)
    send_y(0, (1,))
    send_y(1, (1,))
    plane_heard(2)
    plane_tell(3)

    @pl.when(relay)
    def _():
        zwrap().wait_recv()
        zforward().start()

    def not_(has):
        return lambda side: jnp.logical_not(has(side))

    def wall_y(side):
        sg = 0.5 if side == 0 else -0.5
        for f in (NZ_, NX_, NF_):
            yrecv[side, f] = jnp.zeros((BX, BZ), jnp.float32)
        yrecv[side, NY_] = sg * ysend[side, FP]

    def wall_x(side):
        for f in (VX, VY, VZ):
            xrecv[side, f] = zero
        xrecv[side, PR] = V[PR, pl.ds(BY if side == 0 else ROWS, BY), :]
        FX[pl.ds(0 if side == 0 else ROWS + BY, BY), :] = zero

    when_each(not_(yhas), wall_y)
    when_each(not_(xhas), wall_x)

    when_each(xhas, lambda side: xcopy(1 - side).wait_recv())
    for side in range(2):
        sg = 0.5 if side == 0 else -0.5
        r = BY if side == 0 else ROWS
        g = G[pl.ds(r - BY, BY), :]
        coef = NU + sg * V[VX, pl.ds(r, BY), :]
        for k in range(3):
            n = coef * xrecv[side, k]
            if k == 0:
                n = n + sg * xrecv[side, PR]
            vel_o[k, pl.ds(r - BY, BY), :] += g * n

    for side in range(2):
        zcopy(1 - side, zsend, zrecv, zs, zr).wait_recv()
    for i in range(4):
        ln = pl.ds(BZ * i, BZ)
        vlo, vhi = zsend[0, 2:3, ln], zsend[1, 2:3, ln]
        clo, chi = NU + 0.5 * vlo, NU - 0.5 * vhi
        for k in range(3):
            nlo, nhi = clo * zrecv[0, k:k + 1, ln], chi * zrecv[1, k:k + 1, ln]
            if k == 2:
                nlo = nlo + 0.5 * zrecv[0, 3:4, ln]
                nhi = nhi - 0.5 * zrecv[1, 3:4, ln]
            Q[2 * k:2 * k + 1, ln] = nhi
            Q[2 * k + 1:2 * k + 2, ln] = nlo
        Q[6:7, ln] = zrecv[1, 4:5, ln]
        Q[7:8, ln] = zrecv[0, 4:5, ln]

    def unpack():
        for i in range(4):
            S[pl.ds(BZ * i, BZ), :] = Q[:, pl.ds(BZ * i, BZ)].T

    unpack()
    edge = (lane == 0) | (lane == BZ - 1)

    def zfix(x, carry):
        flow, void = carry
        o = pl.multiple_of(x * BY, BY)
        q, g, e = S[pl.ds(o, BY), :], G[pl.ds(o, BY), :], E[pl.ds(o, BY), :]
        for k in range(3):
            u = vel_o[k, pl.ds(o, BY), :] + g * jnp.where(edge, pltpu.roll(q, BZ - 1 - 2 * k, 1), 0.0)
            vel_o[k, pl.ds(o, BY), :] = u
        h = pltpu.roll(q, BZ - 7, 1)
        SL[pl.ds(o, BY), :] = 0.5 * (
            jnp.where(lane == BZ - 1, h, pltpu.roll(e, BZ - 1, 1))
            - jnp.where(lane == 0, h, pltpu.roll(e, 1, 1))
        )
        return flow + e * u, void + e

    flow, void = lax.fori_loop(0, BX, zfix, (zero, zero), unroll=4)

    for side in range(2):
        rows = pl.ds(face(side), BX, stride=BY)
        ysend[side, FC] = E[rows, :] * vel_o[VY, rows, :]
    send_y(0, (2,))
    send_y(1, (2,))

    yacc[...] = jnp.zeros_like(yacc)

    def couple(k, f, n):
        for q in range(2):
            sg = -0.5 if q == 0 else 0.5
            t = (NU + sg * mrecv[q, FVY]) * mrecv[1 - q, f]
            if k == VY:
                t = t + sg * mrecv[1 - q, FP]
            msend[q, n] = t

    def both(fn):
        for q in range(2):
            fn(q)

    @pl.when(middle)
    def _():
        both(lambda q: mwait(q, 0))
        couple(VZ, FVZ, NZ_)
        yacc[...] = mrecv[0, FD] * msend[0, NZ_] + mrecv[1, FD] * msend[1, NZ_]

    def spread(a, b):
        a, b = jnp.sum(a, axis=0, keepdims=True), jnp.sum(b, axis=0, keepdims=True)
        return jnp.where(
            lane[0:1] < BZ // 2, a + pltpu.roll(a, BZ // 2, 1), b + pltpu.roll(b, BZ // 2, 1)
        )

    part = spread(flow + (yacc[0:16] + yacc[16:32]), void)
    row1[0] = part
    red1[zabs] = part

    def c1(k):
        return remote(row1.at[0], red1.at[zabs], s1, r1, zpeers[k - 1])

    def c2(k):
        return remote(row2.at[0], red2.at[plane], s2, r2, ppeers[k - 1])

    heard(2, 0)
    heard(2, 1)
    for k in range(1, 16):
        c1(k).start()

    @pl.when(middle)
    def _():
        both(lambda q: mcopy(q, 0).start())
        both(lambda q: mwait(q, 1))
        couple(VY, FVY, NY_)
        couple(VX, FVX, NX_)
        both(lambda q: mcopy(q, 1).start())
        both(lambda q: mwait(q, 2))
        for q in range(2):
            msend[q, NF_] = mrecv[1 - q, FC] + mrecv[1 - q, FD] * msend[1 - q, NY_]
        both(lambda q: mcopy(q, 2).start())

    def yback(j, terms):
        when_each(yhas, lambda side: mcopy(1 - side, j).wait_recv())
        for side in range(2):
            rows = pl.ds(face(side), BX, stride=BY)
            g = G[rows, :]
            for k, n in terms:
                vel_o[k, rows, :] = vel_o[k, rows, :] + g * yrecv[side, n]

    yback(0, ((VZ, NZ_),))

    def zflux(x, carry):
        o = pl.multiple_of(x * BY, BY)
        fz = E[pl.ds(o, BY), :] * vel_o[VZ, pl.ds(o, BY), :]
        S[pl.ds(o, BY), :] = jnp.where(lane == 8, pltpu.roll(fz, 9, 1), fz)
        return carry

    lax.fori_loop(0, BX, zflux, 0, unroll=8)
    pack(zsend2)
    for side in range(2):
        zcopy(side, zsend2, zrecv2, zs2, zr2).start()

    def all_of(red, n, a, b):
        return remote(red.at[pl.ds(0, n)], red.at[pl.ds(0, n)], a, b, above[2])

    all_of(red1, 15, s1, r1).wait_recv()
    part2 = red1[0]
    for i in range(1, 16):
        part2 = part2 + red1[i]
    row2[0] = part2
    red2[plane] = part2
    plane_heard(3)
    for k in range(1, 32):
        c2(k).start()

    yback(1, ((VX, NX_), (VY, NY_)))

    def xflux(x, carry):
        o = pl.multiple_of(x * BY, BY)
        FX[pl.ds(o + BY, BY), :] = E[pl.ds(o, BY), :] * vel_o[VX, pl.ds(o, BY), :]
        return carry

    lax.fori_loop(0, BX, xflux, 0, unroll=8)
    for side in range(2):
        xsend2[side] = FX[pl.ds(BY if side == 0 else ROWS, BY), :]

    def xcopy2(side):
        return remote(
            xsend2.at[side], FX.at[pl.ds(ROWS + BY if side == 0 else 0, BY), :],
            xs2.at[side], xr2.at[1 - side], xlow if side == 0 else xhigh,
        )

    when_each(xhas, lambda side: xcopy2(side).start())

    when_each(yhas, lambda side: mcopy(1 - side, 2).wait_recv())
    for side in range(2):
        zcopy(1 - side, zsend2, zrecv2, zs2, zr2).wait_recv()
    Q[0:1, :] = zrecv2[1, 0:1, :]
    Q[1:2, :] = zrecv2[0, 0:1, :]
    unpack()
    when_each(xhas, lambda side: xcopy2(1 - side).wait_recv())

    def diverge(x, carry):
        o = pl.multiple_of(x * BY, BY)
        e = E[pl.ds(o, BY), :]
        fy = e * vel_o[VY, pl.ds(o, BY), :]
        fz = e * vel_o[VZ, pl.ds(o, BY), :]
        h = pltpu.roll(S[pl.ds(o, BY), :], BZ - 1, 1)
        d = FX[pl.ds(o + 2 * BY, BY), :] - FX[pl.ds(o, BY), :]
        d = d + (
            jnp.where(rown == BY - 1, yrecv[1, NF_, pl.ds(x, 1), :], pltpu.roll(fy, BY - 1, 0))
            - jnp.where(rown == 0, yrecv[0, NF_, pl.ds(x, 1), :], pltpu.roll(fy, 1, 0))
        )
        d = d + (
            jnp.where(lane == BZ - 1, h, pltpu.roll(fz, BZ - 1, 1))
            - jnp.where(lane == 0, h, pltpu.roll(fz, 1, 1))
        )
        src_o[pl.ds(o, BY), :] = 0.5 * d
        return carry

    lax.fori_loop(0, BX, diverge, 0, unroll=4)

    all_of(red2, 31, s2, r2).wait_recv()
    total = red2[0]
    for i in range(1, 32):
        total = total + red2[i]
    half = lane[0:1] < BZ // 2
    flow_sum = jnp.sum(jnp.where(half, total, 0.0), axis=1, keepdims=True)
    void_sum = jnp.sum(jnp.where(half, 0.0, total), axis=1, keepdims=True)
    cells = float(ROWS * BZ * 512)
    step = (target * cells - flow_sum) / (DT * void_sum)
    aux_o[0:1, :] = jnp.broadcast_to(DT * step, (1, BZ))
    aux_o[1:2, :] = jnp.broadcast_to(force + step, (1, BZ))

    for kind in range(2):
        @pl.when(paired(kind))
        def _():
            for j in range(3):
                ycopy(kind, j).wait_send()

    @pl.when(middle)
    def _():
        both(lambda q: [mcopy(q, j).wait_send() for j in range(3)])

    when_each(xhas, lambda side: (xcopy(side).wait_send(), xcopy2(side).wait_send()) and None)
    @pl.when(relay)
    def _():
        zforward().wait_send()

    for side in range(2):
        zcopy(side, zsend, zrecv, zs, zr).wait_send()
        zcopy(side, zsend2, zrecv2, zs2, zr2).wait_send()
    all_of(red1, 15, s1, r1).wait_send()
    all_of(red2, 31, s2, r2).wait_send()


def finish(vel, src, slope, aux, vel_o, src_o, force_o, vz, out, sem):
    pairs = [
        pltpu.make_async_copy(vel.at[pl.ds(0, 2)], vel_o.at[pl.ds(0, 2)], sem.at[0]),
        pltpu.make_async_copy(vz, vel_o.at[VZ], sem.at[1]),
        pltpu.make_async_copy(out, src_o, sem.at[2]),
    ]
    pairs[0].start()
    force_o[...] = aux[1:2, 0:1]
    add = aux[0:1, :]
    vz[...] = vel[VZ] + add
    pairs[1].start()
    out[...] = src[...] + add * slope[...]
    pairs[2].start()
    for cp in pairs:
        cp.wait()


def local(velocity, pressure, voidage, particle_vel, forcing, target_flux):
    f32 = jnp.float32
    vmem = pl.BlockSpec(memory_space=pltpu.VMEM)
    hbm = pl.BlockSpec(memory_space=pl.ANY)
    dma = pltpu.SemaphoreType.DMA
    parts = pl.pallas_call(
        kernel,
        out_shape=(
            pltpu.VMEM((3, ROWS, BZ), f32),
            pltpu.VMEM((ROWS, BZ), f32),
            pltpu.VMEM((ROWS, BZ), f32),
            pltpu.VMEM((8, BZ), f32),
        ),
        in_specs=[pl.BlockSpec(memory_space=pltpu.HBM)] * 6,
        out_specs=(vmem,) * 4,
        scratch_shapes=[
            pltpu.VMEM((4, PAD, BZ), f32),
            pltpu.VMEM((ROWS, BZ), f32),
            pltpu.VMEM((3, ROWS, BZ), f32),
            pltpu.VMEM((ROWS, BZ), f32),
            pltpu.VMEM((ROWS, BZ), f32),
            pltpu.VMEM((PAD, BZ), f32),
            pltpu.VMEM((BZ, ROWS), f32),
            pltpu.SMEM((2, 1), f32),
            pltpu.VMEM((2, 4, BY, BZ), f32),
            pltpu.VMEM((2, 8, ROWS), f32),
            pltpu.VMEM((2, 8, ROWS), f32),
            pltpu.VMEM((2, 8, ROWS), f32),
            pltpu.VMEM((2, 8, ROWS), f32),
            pltpu.VMEM((2, 6, BX, BZ), f32),
            pltpu.VMEM((2, 4, BX, BZ), f32),
            pltpu.VMEM((2, 4, BX, BZ), f32),
            pltpu.VMEM((2, 6, BX, BZ), f32),
            pltpu.VMEM((BX, BZ), f32),
            pltpu.VMEM((2, BY, BZ), f32),
            pltpu.VMEM((8, ROWS), f32),
            pltpu.VMEM((1, 1, BZ), f32),
            pltpu.VMEM((16, 1, BZ), f32),
            pltpu.VMEM((1, 1, BZ), f32),
            pltpu.VMEM((32, 1, BZ), f32),
            dma((6,)), dma((2,)), dma((2,)), dma((2,)), dma((2,)), dma((2,)), dma((2,)),
            dma((2, 3)), dma((2, 3)), dma((2, 3)), dma((2, 3)), dma((2,)), dma((2,)),
            dma, dma, dma, dma, pltpu.SemaphoreType.REGULAR((3, 2)), pltpu.SemaphoreType.REGULAR((4,)),
            pltpu.SemaphoreType.REGULAR, dma, dma,
        ],
        compiler_params=pltpu.CompilerParams(collective_id=0, has_side_effects=True),
    )(
        forcing,
        target_flux,
        velocity.reshape(3, ROWS, BZ),
        pressure.reshape(ROWS, BZ),
        voidage.reshape(ROWS, BZ),
        particle_vel.reshape(3, ROWS, BZ),
    )
    vel, src, force = pl.pallas_call(
        finish,
        out_shape=(
            jax.ShapeDtypeStruct((3, ROWS, BZ), f32),
            jax.ShapeDtypeStruct((ROWS, BZ), f32),
            jax.ShapeDtypeStruct((1, 1), f32),
        ),
        in_specs=[vmem] * 4,
        out_specs=(hbm, hbm, vmem),
        scratch_shapes=[pltpu.VMEM((ROWS, BZ), f32), pltpu.VMEM((ROWS, BZ), f32), dma((3,))],
        compiler_params=pltpu.CompilerParams(vmem_limit_bytes=8 * 1024 * 1024),
    )(*[pltpu.with_memory_space_constraint(p, pltpu.VMEM) for p in parts])
    return vel.reshape(3, BX, BY, BZ), src.reshape(BX, BY, BZ), force.reshape(1)


def solution(mesh):
    return jax.shard_map(
        local,
        mesh=mesh,
        in_specs=(
            P(None, "gx", "gy", "gz"), P("gx", "gy", "gz"), P("gx", "gy", "gz"),
            P(None, "gx", "gy", "gz"), P(), P(),
        ),
        out_specs=(P(None, "gx", "gy", "gz"), P("gx", "gy", "gz"), P()),
        check_vma=False,
    )
```

```python
import jax
import jax.numpy as jnp
from jax import lax
from jax.experimental import pallas as pl
from jax.experimental.pallas import tpu as pltpu
from jax.sharding import PartitionSpec as P

MESH = pl.DeviceIdType.MESH
DT = 0.2
NU = 0.1
BX, BY, BZ = 32, 16, 128
ROWS = BX * BY
PAD = ROWS + 2 * BY
VX, VY, VZ, PR = 0, 1, 2, 3
FVZ, FVY, FD, FP, FVX, FC = 0, 1, 2, 3, 4, 5
GROUPS = ((0, 3), (3, 2), (5, 1))
NZ_, NY_, NX_, NF_ = 0, 1, 2, 3
BACK = ((0, 1), (1, 2), (3, 1))


def weight(c, pv, e):
    a, b, d = c[0] - pv[0], c[1] - pv[1], c[2] - pv[2]
    slip = jnp.sqrt(a * a + b * b + d * d)
    drag = (1.0 - e) * jnp.exp(-2.65 * jnp.log(e)) * (1.0 + slip)
    return drag, 1.0 / (1.0 + DT * drag)


def kernel(
    force_h, target_h, vel_h, pres_h, eps_h, pv_h,
    vel_o, src_o, SL, aux_o,
    V, E, PV, G, S, FX, Q, scal,
    xrecv, zsend, zrecv, zsend2, zrecv2, ysend, yrecv, msend, mrecv, yacc, xsend2, rbuf,
    row1, red1, row2, red2,
    lsem, xs, xr, zs, zr, zs2, zr2, ys, yr, ms, mr, xs2, xr2, s1, r1, s2, r2, know, wave, rsem, fsem,
):
    gz, gy, gx = lax.axis_index("gz"), lax.axis_index("gy"), lax.axis_index("gx")
    ngz, ngy, ngx = 16, 8, 4
    here = {"gz": gz, "gy": gy, "gx": gx}

    def at(**kw):
        return {**here, **kw}

    y, zhi = gy // 2, gy % 2
    zlo, core = gz // 2, gz % 2
    zabs = zhi * 8 + zlo
    xi, yi = gx, y
    has_xlo, has_xhi = gx > 0, gx < ngx - 1
    has_ylo, has_yhi = gy > 0, gy < ngy - 1

    def of_z(z, dy=0):
        z, yy = lax.rem(z, 16), lax.rem(y + dy + 4, 4)
        return at(gz=lax.rem(z, 8) * 2 + core, gy=yy * 2 + z // 8)

    def of_plane(i):
        return at(gx=i // 8, gy=lax.rem(i // 2, 4) * 2 + zhi, gz=zlo * 2 + lax.rem(i, 2))

    plane = gx * 8 + y * 2 + core
    zpeers = [of_z(zabs + k) for k in range(1, 16)]
    ppeers = [of_plane(lax.rem(plane + k, 32)) for k in range(1, 32)]
    zlow, zhigh = at(gz=lax.rem(gz + ngz - 1, ngz)), at(gz=lax.rem(gz + 1, ngz))
    xlow, xhigh = at(gx=lax.rem(gx + ngx - 1, ngx)), at(gx=lax.rem(gx + 1, ngx))

    barrier = pltpu.get_barrier_semaphore()
    yprev, ynext = of_z(zabs, -1), of_z(zabs, 1)
    other = at(gz=zlo * 2 + 1 - core)
    outer_far = (gz == 0) | (gz == ngz - 1)
    outer = at(gz=lax.rem(gz + ngz - 1 + 2 * core, ngz))
    across_z = lax.rem(zabs + 19 - 6 * core, 16)
    across = at(gz=lax.rem(across_z, 8) * 2 + 1 - core, gy=y * 2 + across_z // 8)
    nearest = [of_z(zabs + 16 + k) for k in (-4, 4, -3, 3, -2, 2, -1, 1)]
    below, above = nearest[:2]
    nearest += [of_z(zabs + 4, 1), of_z(zabs + 12, -1), across]
    nearest += [xlow, xhigh, yprev, ynext, other]
    for d in nearest:
        pl.semaphore_signal(barrier, inc=1, device_id=d, device_id_type=MESH)

    @pl.when(jnp.logical_not(outer_far))
    def _():
        pl.semaphore_signal(barrier, inc=1, device_id=outer, device_id_type=MESH)

    loads = [
        pltpu.make_async_copy(vel_h, V.at[pl.ds(0, 3), pl.ds(BY, ROWS), :], lsem.at[0]),
        pltpu.make_async_copy(pres_h, V.at[3, pl.ds(BY, ROWS), :], lsem.at[1]),
        pltpu.make_async_copy(eps_h, E, lsem.at[2]),
        pltpu.make_async_copy(pv_h, PV, lsem.at[3]),
        pltpu.make_async_copy(force_h, scal.at[0], lsem.at[4]),
        pltpu.make_async_copy(target_h, scal.at[1], lsem.at[5]),
    ]
    for cp in loads:
        cp.start()

    lane = lax.broadcasted_iota(jnp.int32, (BY, BZ), 1)
    rown = lax.broadcasted_iota(jnp.int32, (BY, BZ), 0)
    zero = jnp.zeros((BY, BZ), jnp.float32)
    for f in range(4):
        V[f, pl.ds(0, BY), :] = zero
        V[f, pl.ds(ROWS + BY, BY), :] = zero
    Q[...] = jnp.zeros_like(Q)
    for cp in loads:
        cp.wait()
    force, target = scal[0, 0], scal[1, 0]

    def face(side):
        return 0 if side == 0 else BY - 1

    for side in range(2):
        rows = pl.ds(face(side), BX, stride=BY)
        v = [V[f, pl.ds(BY + face(side), BX, stride=BY), :] for f in range(4)]
        ysend[side, FVZ], ysend[side, FVY] = v[VZ], v[VY]
        ysend[side, FP], ysend[side, FVX] = v[PR], v[VX]
        e = E[rows, :]
        ysend[side, FD] = e * DT * weight(v, [PV[k, rows, :] for k in range(3)], e)[1]

    def remote(src, dst, a, b, dev):
        return pltpu.make_async_remote_copy(
            src_ref=src, dst_ref=dst, send_sem=a, recv_sem=b, device_id=dev, device_id_type=MESH
        )

    def side_of(kind):
        return 1 - zhi if kind == 0 else zhi

    def ycopy(kind, j):
        side, part = side_of(kind), pl.ds(*GROUPS[j])
        return remote(
            ysend.at[side, part], mrecv.at[1 - side, part], ys.at[kind, j], mr.at[1 - side, j],
            of_z(zabs + 12 + 8 * side, kind * zhi),
        )

    def paired(kind):
        return (gy >= 0) if kind == 0 else jnp.where(zhi == 0, y, 3 - y) > 0

    def mwait(q, j):
        part = pl.ds(*GROUPS[j])
        remote(ysend.at[0, part], mrecv.at[q, part], ys.at[0, j], mr.at[q, j], above).wait_recv()

    def yhas(side):
        return has_ylo if side == 0 else has_yhi

    intra = (zabs >= 4) & (zabs < 12)
    middle = intra | (y > 0)

    def mcopy(q, j):
        part = pl.ds(*BACK[j])
        return remote(
            msend.at[q, part], yrecv.at[1 - q, part], ms.at[q, j], yr.at[1 - q, j],
            of_z(zabs + 12, jnp.where(intra, 0, -1)) if q == 0 else of_z(zabs + 4),
        )

    def xcopy(side):
        r = BY if side == 0 else ROWS
        return remote(
            V.at[:, pl.ds(r, BY), :], xrecv.at[1 - side], xs.at[side], xr.at[1 - side],
            xlow if side == 0 else xhigh,
        )

    def xhas(side):
        return has_xlo if side == 0 else has_xhi

    def zcopy(side, src, dst, a, b):
        return remote(
            src.at[side], dst.at[1 - side], a.at[side], b.at[1 - side],
            zlow if side == 0 else zhigh,
        )

    def when_each(has, fn):
        for side in range(2):
            pl.when(has(side))(lambda side=side: fn(side))

    def send_y(kind, groups):
        @pl.when(paired(kind))
        def _():
            for g in groups:
                ycopy(kind, g).start()

    def heard():
        pl.semaphore_wait(know.at[0], 1)
        pl.semaphore_wait(know.at[1], 1)

    waves = [(xlow, xhigh), (yprev, ynext), (yprev, ynext), (other,)]

    def plane_tell(i):
        for d in waves[i]:
            pl.semaphore_signal(wave.at[i], inc=1, device_id=d, device_id_type=MESH)

    def plane_heard(i):
        pl.semaphore_wait(wave.at[i], len(waves[i]))

    def columns(x, carry):
        o = pl.multiple_of(x * BY, BY)
        s = zero
        for k, a in enumerate([V[f, pl.ds(o + BY, BY), :] for f in range(4)] + [E[pl.ds(o, BY), :]]):
            s = jnp.where(lane == k, a if k == 0 else pltpu.roll(a, k, 1), s)
            s = jnp.where(lane == 8 + k, pltpu.roll(a, 9 + k, 1), s)
        S[pl.ds(o, BY), :] = s
        return carry

    lax.fori_loop(0, BX, columns, 0, unroll=4)

    def pack(dst, n):
        for i in range(4):
            t = S[pl.ds(BZ * i, BZ), :].T
            dst[0, :, pl.ds(BZ * i, BZ)] = t[0:n]
            dst[1, :, pl.ds(BZ * i, BZ)] = t[8:8 + n]

    pack(zsend, 8)
    relay = zlo == 4 - core

    def zwrap():
        return remote(
            zsend.at[core], rbuf, zs.at[core], rsem, of_z(zabs + 20 - 8 * core),
        )

    def zforward():
        return remote(
            rbuf, zrecv.at[1 - core], fsem, zr.at[1 - core], at(gz=gz + 7 - 14 * core),
        )

    pl.semaphore_wait(barrier, len(nearest) + jnp.where(outer_far, 0, 1))
    @pl.when(outer_far)
    def _():
        zwrap().start()

    for side in range(2):
        @pl.when(jnp.logical_not(outer_far & (core == side)))
        def _():
            zcopy(side, zsend, zrecv, zs, zr).start()

    send_y(0, (0,))
    send_y(1, (0,))
    when_each(xhas, lambda side: xcopy(side).start())

    pl.semaphore_signal(know.at[0], inc=1, device_id=above, device_id_type=MESH)
    pl.semaphore_signal(know.at[1], inc=1, device_id=below, device_id_type=MESH)
    plane_tell(0)

    def slab(x, carry):
        o = pl.multiple_of(x * BY, BY)
        c = [V[f, pl.ds(o + BY, BY), :] for f in range(4)]
        xm = [V[f, pl.ds(o, BY), :] for f in range(4)]
        xp = [V[f, pl.ds(o + 2 * BY, BY), :] for f in range(4)]
        e = E[pl.ds(o, BY), :]
        pv = [PV[k, pl.ds(o, BY), :] for k in range(3)]
        zm = [jnp.where(lane == 0, 0.0, pltpu.roll(a, 1, 1)) for a in c]
        zp = [jnp.where(lane == BZ - 1, 0.0, pltpu.roll(a, BZ - 1, 1)) for a in c]
        ym = [jnp.where(rown == 0, 0.0, pltpu.roll(a, 1, 0)) for a in c]
        yp = [jnp.where(rown == BY - 1, 0.0, pltpu.roll(a, BY - 1, 0)) for a in c]
        drag, w = weight(c, pv, e)
        hi, lo = (xp, yp, zp), (xm, ym, zm)
        for k in range(3):
            adv = zero
            lap = -6.0 * c[k]
            for d in range(3):
                adv = adv + c[d] * (hi[d][k] - lo[d][k])
                lap = lap + hi[d][k] + lo[d][k]
            fk = NU * lap - 0.5 * (adv + (hi[k][3] - lo[k][3]))
            if k == 2:
                fk = fk + force
            vel_o[k, pl.ds(o, BY), :] = (c[k] + DT * (fk + drag * pv[k])) * w
        G[pl.ds(o, BY), :] = DT * w
        return carry

    lax.fori_loop(0, BX, slab, 0, unroll=4)
    plane_heard(0)
    plane_tell(1)

    @pl.when(outer_far)
    def _():
        send_y(0, (1,))
        send_y(1, (1,))

    @pl.when(relay)
    def _():
        zwrap().wait_recv()
        zforward().start()

    plane_heard(1)
    plane_tell(2)

    def not_(has):
        return lambda side: jnp.logical_not(has(side))

    def wall_y(side):
        sg = 0.5 if side == 0 else -0.5
        for f in (NZ_, NX_, NF_):
            yrecv[side, f] = jnp.zeros((BX, BZ), jnp.float32)
        yrecv[side, NY_] = sg * ysend[side, FP]

    def wall_x(side):
        for f in (VX, VY, VZ):
            xrecv[side, f] = zero
        xrecv[side, PR] = V[PR, pl.ds(BY if side == 0 else ROWS, BY), :]
        FX[pl.ds(0 if side == 0 else ROWS + BY, BY), :] = zero

    when_each(not_(yhas), wall_y)
    when_each(not_(xhas), wall_x)

    when_each(xhas, lambda side: xcopy(1 - side).wait_recv())
    for side in range(2):
        sg = 0.5 if side == 0 else -0.5
        r = BY if side == 0 else ROWS
        g = G[pl.ds(r - BY, BY), :]
        coef = NU + sg * V[VX, pl.ds(r, BY), :]
        for k in range(3):
            n = coef * xrecv[side, k]
            if k == 0:
                n = n + sg * xrecv[side, PR]
            vel_o[k, pl.ds(r - BY, BY), :] += g * n

    for side in range(2):
        zcopy(1 - side, zsend, zrecv, zs, zr).wait_recv()
    for i in range(4):
        ln = pl.ds(BZ * i, BZ)
        vlo, vhi = zsend[0, 2:3, ln], zsend[1, 2:3, ln]
        clo, chi = NU + 0.5 * vlo, NU - 0.5 * vhi
        for k in range(3):
            nlo, nhi = clo * zrecv[0, k:k + 1, ln], chi * zrecv[1, k:k + 1, ln]
            if k == 2:
                nlo = nlo + 0.5 * zrecv[0, 3:4, ln]
                nhi = nhi - 0.5 * zrecv[1, 3:4, ln]
            Q[2 * k:2 * k + 1, ln] = nhi
            Q[2 * k + 1:2 * k + 2, ln] = nlo
        Q[6:7, ln] = zrecv[1, 4:5, ln]
        Q[7:8, ln] = zrecv[0, 4:5, ln]

    def unpack():
        for i in range(4):
            S[pl.ds(BZ * i, BZ), :] = Q[:, pl.ds(BZ * i, BZ)].T

    unpack()
    edge = (lane == 0) | (lane == BZ - 1)

    def zfix(x, carry):
        flow, void = carry
        o = pl.multiple_of(x * BY, BY)
        q, g, e = S[pl.ds(o, BY), :], G[pl.ds(o, BY), :], E[pl.ds(o, BY), :]
        for k in range(3):
            u = vel_o[k, pl.ds(o, BY), :] + g * jnp.where(edge, pltpu.roll(q, BZ - 1 - 2 * k, 1), 0.0)
            vel_o[k, pl.ds(o, BY), :] = u
        h = pltpu.roll(q, BZ - 7, 1)
        SL[pl.ds(o, BY), :] = 0.5 * (
            jnp.where(lane == BZ - 1, h, pltpu.roll(e, BZ - 1, 1))
            - jnp.where(lane == 0, h, pltpu.roll(e, 1, 1))
        )
        return flow + e * u, void + e

    flow, void = lax.fori_loop(0, BX, zfix, (zero, zero), unroll=4)

    for side in range(2):
        rows = pl.ds(face(side), BX, stride=BY)
        ysend[side, FC] = E[rows, :] * vel_o[VY, rows, :]
    plane_heard(2)
    plane_tell(3)

    @pl.when(jnp.logical_not(outer_far))
    def _():
        send_y(0, (1,))
        send_y(1, (1,))

    send_y(0, (2,))
    send_y(1, (2,))

    yacc[...] = jnp.zeros_like(yacc)

    def couple(k, f, n):
        for q in range(2):
            sg = -0.5 if q == 0 else 0.5
            t = (NU + sg * mrecv[q, FVY]) * mrecv[1 - q, f]
            if k == VY:
                t = t + sg * mrecv[1 - q, FP]
            msend[q, n] = t

    def both(fn):
        for q in range(2):
            fn(q)

    @pl.when(middle)
    def _():
        both(lambda q: mwait(q, 0))
        couple(VZ, FVZ, NZ_)
        yacc[...] = mrecv[0, FD] * msend[0, NZ_] + mrecv[1, FD] * msend[1, NZ_]

    def spread(a, b):
        a, b = jnp.sum(a, axis=0, keepdims=True), jnp.sum(b, axis=0, keepdims=True)
        return jnp.where(
            lane[0:1] < BZ // 2, a + pltpu.roll(a, BZ // 2, 1), b + pltpu.roll(b, BZ // 2, 1)
        )

    part = spread(flow + (yacc[0:16] + yacc[16:32]), void)
    row1[0] = part
    red1[zabs] = part

    def c1(k):
        return remote(row1.at[0], red1.at[zabs], s1, r1, zpeers[k - 1])

    def c2(k):
        return remote(row2.at[0], red2.at[plane], s2, r2, ppeers[k - 1])

    heard()
    for k in range(1, 16):
        c1(k).start()

    @pl.when(middle)
    def _():
        both(lambda q: mcopy(q, 0).start())
        both(lambda q: mwait(q, 1))
        couple(VY, FVY, NY_)
        couple(VX, FVX, NX_)
        both(lambda q: mcopy(q, 1).start())

    @pl.when(middle)
    def _():
        both(lambda q: mwait(q, 2))
        for q in range(2):
            msend[q, NF_] = mrecv[1 - q, FC] + mrecv[1 - q, FD] * msend[1 - q, NY_]
        both(lambda q: mcopy(q, 2).start())

    def all_of(red, n, a, b):
        return remote(red.at[pl.ds(0, n)], red.at[pl.ds(0, n)], a, b, above)

    all_of(red1, 15, s1, r1).wait_recv()
    part2 = red1[0]
    for i in range(1, 16):
        part2 = part2 + red1[i]
    row2[0] = part2
    red2[plane] = part2
    plane_heard(3)
    for k in range(1, 32):
        c2(k).start()

    def yback(j, terms):
        when_each(yhas, lambda side: mcopy(1 - side, j).wait_recv())
        for side in range(2):
            rows = pl.ds(face(side), BX, stride=BY)
            g = G[rows, :]
            for k, n in terms:
                vel_o[k, rows, :] = vel_o[k, rows, :] + g * yrecv[side, n]

    yback(0, ((VZ, NZ_),))

    def zflux(x, carry):
        o = pl.multiple_of(x * BY, BY)
        fz = E[pl.ds(o, BY), :] * vel_o[VZ, pl.ds(o, BY), :]
        S[pl.ds(o, BY), :] = jnp.where(lane == 8, pltpu.roll(fz, 9, 1), fz)
        return carry

    lax.fori_loop(0, BX, zflux, 0, unroll=8)
    pack(zsend2, 1)
    for side in range(2):
        zcopy(side, zsend2, zrecv2, zs2, zr2).start()

    yback(1, ((VX, NX_), (VY, NY_)))

    def xflux(x, carry):
        o = pl.multiple_of(x * BY, BY)
        FX[pl.ds(o + BY, BY), :] = E[pl.ds(o, BY), :] * vel_o[VX, pl.ds(o, BY), :]
        return carry

    lax.fori_loop(0, BX, xflux, 0, unroll=8)
    for side in range(2):
        xsend2[side] = FX[pl.ds(BY if side == 0 else ROWS, BY), :]

    def xcopy2(side):
        return remote(
            xsend2.at[side], FX.at[pl.ds(ROWS + BY if side == 0 else 0, BY), :],
            xs2.at[side], xr2.at[1 - side], xlow if side == 0 else xhigh,
        )

    when_each(xhas, lambda side: xcopy2(side).start())

    when_each(yhas, lambda side: mcopy(1 - side, 2).wait_recv())
    for side in range(2):
        zcopy(1 - side, zsend2, zrecv2, zs2, zr2).wait_recv()
    Q[0:1, :] = zrecv2[1, 0:1, :]
    Q[1:2, :] = zrecv2[0, 0:1, :]
    unpack()
    when_each(xhas, lambda side: xcopy2(1 - side).wait_recv())

    def diverge(x, carry):
        o = pl.multiple_of(x * BY, BY)
        e = E[pl.ds(o, BY), :]
        fy = e * vel_o[VY, pl.ds(o, BY), :]
        fz = e * vel_o[VZ, pl.ds(o, BY), :]
        h = pltpu.roll(S[pl.ds(o, BY), :], BZ - 1, 1)
        d = FX[pl.ds(o + 2 * BY, BY), :] - FX[pl.ds(o, BY), :]
        d = d + (
            jnp.where(rown == BY - 1, yrecv[1, NF_, pl.ds(x, 1), :], pltpu.roll(fy, BY - 1, 0))
            - jnp.where(rown == 0, yrecv[0, NF_, pl.ds(x, 1), :], pltpu.roll(fy, 1, 0))
        )
        d = d + (
            jnp.where(lane == BZ - 1, h, pltpu.roll(fz, BZ - 1, 1))
            - jnp.where(lane == 0, h, pltpu.roll(fz, 1, 1))
        )
        src_o[pl.ds(o, BY), :] = 0.5 * d
        return carry

    lax.fori_loop(0, BX, diverge, 0, unroll=4)

    all_of(red2, 31, s2, r2).wait_recv()
    total = red2[0]
    for i in range(1, 32):
        total = total + red2[i]
    half = lane[0:1] < BZ // 2
    flow_sum = jnp.sum(jnp.where(half, total, 0.0), axis=1, keepdims=True)
    void_sum = jnp.sum(jnp.where(half, 0.0, total), axis=1, keepdims=True)
    cells = float(ROWS * BZ * 512)
    step = (target * cells - flow_sum) / (DT * void_sum)
    aux_o[0:1, :] = jnp.broadcast_to(DT * step, (1, BZ))
    aux_o[1:2, :] = jnp.broadcast_to(force + step, (1, BZ))

    for kind in range(2):
        @pl.when(paired(kind))
        def _():
            for j in range(3):
                ycopy(kind, j).wait_send()

    @pl.when(middle)
    def _():
        both(lambda q: [mcopy(q, j).wait_send() for j in range(3)])

    when_each(xhas, lambda side: (xcopy(side).wait_send(), xcopy2(side).wait_send()) and None)
    @pl.when(relay)
    def _():
        zforward().wait_send()

    for side in range(2):
        zcopy(side, zsend, zrecv, zs, zr).wait_send()
        zcopy(side, zsend2, zrecv2, zs2, zr2).wait_send()
    all_of(red1, 15, s1, r1).wait_send()
    all_of(red2, 31, s2, r2).wait_send()


def finish(vel, src, slope, aux, vel_o, src_o, force_o, vz, out, sem):
    pairs = [
        pltpu.make_async_copy(vel.at[pl.ds(0, 2)], vel_o.at[pl.ds(0, 2)], sem.at[0]),
        pltpu.make_async_copy(vz, vel_o.at[VZ], sem.at[1]),
        pltpu.make_async_copy(out, src_o, sem.at[2]),
    ]
    pairs[0].start()
    force_o[...] = aux[1:2, 0:1]
    add = aux[0:1, :]
    vz[...] = vel[VZ] + add
    pairs[1].start()
    out[...] = src[...] + add * slope[...]
    pairs[2].start()
    for cp in pairs:
        cp.wait()


def local(velocity, pressure, voidage, particle_vel, forcing, target_flux):
    f32 = jnp.float32
    vmem = pl.BlockSpec(memory_space=pltpu.VMEM)
    hbm = pl.BlockSpec(memory_space=pl.ANY)
    dma = pltpu.SemaphoreType.DMA
    parts = pl.pallas_call(
        kernel,
        out_shape=(
            pltpu.VMEM((3, ROWS, BZ), f32),
            pltpu.VMEM((ROWS, BZ), f32),
            pltpu.VMEM((ROWS, BZ), f32),
            pltpu.VMEM((8, BZ), f32),
        ),
        in_specs=[pl.BlockSpec(memory_space=pltpu.HBM)] * 6,
        out_specs=(vmem,) * 4,
        scratch_shapes=[
            pltpu.VMEM((4, PAD, BZ), f32),
            pltpu.VMEM((ROWS, BZ), f32),
            pltpu.VMEM((3, ROWS, BZ), f32),
            pltpu.VMEM((ROWS, BZ), f32),
            pltpu.VMEM((ROWS, BZ), f32),
            pltpu.VMEM((PAD, BZ), f32),
            pltpu.VMEM((BZ, ROWS), f32),
            pltpu.SMEM((2, 1), f32),
            pltpu.VMEM((2, 4, BY, BZ), f32),
            pltpu.VMEM((2, 8, ROWS), f32),
            pltpu.VMEM((2, 8, ROWS), f32),
            pltpu.VMEM((2, 1, ROWS), f32),
            pltpu.VMEM((2, 1, ROWS), f32),
            pltpu.VMEM((2, 6, BX, BZ), f32),
            pltpu.VMEM((2, 4, BX, BZ), f32),
            pltpu.VMEM((2, 4, BX, BZ), f32),
            pltpu.VMEM((2, 6, BX, BZ), f32),
            pltpu.VMEM((BX, BZ), f32),
            pltpu.VMEM((2, BY, BZ), f32),
            pltpu.VMEM((8, ROWS), f32),
            pltpu.VMEM((1, 1, BZ), f32),
            pltpu.VMEM((16, 1, BZ), f32),
            pltpu.VMEM((1, 1, BZ), f32),
            pltpu.VMEM((32, 1, BZ), f32),
            dma((6,)), dma((2,)), dma((2,)), dma((2,)), dma((2,)), dma((2,)), dma((2,)),
            dma((2, 3)), dma((2, 3)), dma((2, 3)), dma((2, 3)), dma((2,)), dma((2,)),
            dma, dma, dma, dma, pltpu.SemaphoreType.REGULAR((2,)), pltpu.SemaphoreType.REGULAR((4,)), dma, dma,
        ],
        compiler_params=pltpu.CompilerParams(collective_id=0, has_side_effects=True),
    )(
        forcing,
        target_flux,
        velocity.reshape(3, ROWS, BZ),
        pressure.reshape(ROWS, BZ),
        voidage.reshape(ROWS, BZ),
        particle_vel.reshape(3, ROWS, BZ),
    )
    vel, src, force = pl.pallas_call(
        finish,
        out_shape=(
            jax.ShapeDtypeStruct((3, ROWS, BZ), f32),
            jax.ShapeDtypeStruct((ROWS, BZ), f32),
            jax.ShapeDtypeStruct((1, 1), f32),
        ),
        in_specs=[vmem] * 4,
        out_specs=(hbm, hbm, vmem),
        scratch_shapes=[pltpu.VMEM((ROWS, BZ), f32), pltpu.VMEM((ROWS, BZ), f32), dma((3,))],
        compiler_params=pltpu.CompilerParams(vmem_limit_bytes=8 * 1024 * 1024),
    )(*[pltpu.with_memory_space_constraint(p, pltpu.VMEM) for p in parts])
    return vel.reshape(3, BX, BY, BZ), src.reshape(BX, BY, BZ), force.reshape(1)


def solution(mesh):
    return jax.shard_map(
        local,
        mesh=mesh,
        in_specs=(
            P(None, "gx", "gy", "gz"), P("gx", "gy", "gz"), P("gx", "gy", "gz"),
            P(None, "gx", "gy", "gz"), P(), P(),
        ),
        out_specs=(P(None, "gx", "gy", "gz"), P("gx", "gy", "gz"), P()),
        check_vma=False,
    )
```

```python
import jax
import jax.numpy as jnp
from jax import lax
from jax.experimental import pallas as pl
from jax.experimental.pallas import tpu as pltpu
from jax.sharding import PartitionSpec as P

MESH = pl.DeviceIdType.MESH
DT = 0.2
NU = 0.1
BX, BY, BZ = 32, 16, 128
ROWS = BX * BY
PAD = ROWS + 2 * BY
VX, VY, VZ, PR = 0, 1, 2, 3
FVZ, FVY, FD, FP, FVX, FC = 0, 1, 2, 3, 4, 5
GROUPS = ((0, 3), (3, 2), (5, 1))
NZ_, NY_, NX_, NF_ = 0, 1, 2, 3
BACK = ((0, 1), (1, 2), (3, 1))


def weight(c, pv, e):
    a, b, d = c[0] - pv[0], c[1] - pv[1], c[2] - pv[2]
    slip = jnp.sqrt(a * a + b * b + d * d)
    drag = (1.0 - e) * jnp.exp(-2.65 * jnp.log(e)) * (1.0 + slip)
    return drag, 1.0 / (1.0 + DT * drag)


def kernel(
    force_h, target_h, vel_h, pres_h, eps_h, pv_h,
    vel_o, src_o, SL, aux_o, S,
    V, E, PV, G, FX, Q, scal,
    xrecv, zsend, zrecv, zsend2, zrecv2, ysend, yrecv, msend, mrecv, yacc, xsend2, rbuf,
    row1, red1, row2, red2,
    lsem, xs, xr, zs, zr, zs2, zr2, ys, yr, ms, mr, xs2, xr2, s1, r1, s2, r2, know, wave, rsem, fsem,
):
    gz, gy, gx = lax.axis_index("gz"), lax.axis_index("gy"), lax.axis_index("gx")
    ngz, ngy, ngx = 16, 8, 4
    here = {"gz": gz, "gy": gy, "gx": gx}

    def at(**kw):
        return {**here, **kw}

    y, zhi = gy // 2, gy % 2
    zlo, core = gz // 2, gz % 2
    zabs = zhi * 8 + zlo
    xi, yi = gx, y
    has_xlo, has_xhi = gx > 0, gx < ngx - 1
    has_ylo, has_yhi = gy > 0, gy < ngy - 1

    def of_z(z, dy=0):
        z, yy = lax.rem(z, 16), lax.rem(y + dy + 4, 4)
        return at(gz=lax.rem(z, 8) * 2 + core, gy=yy * 2 + z // 8)

    def of_plane(i):
        return at(gx=i // 8, gy=lax.rem(i // 2, 4) * 2 + zhi, gz=zlo * 2 + lax.rem(i, 2))

    plane = gx * 8 + y * 2 + core
    zpeers = [of_z(zabs + k) for k in range(1, 16)]
    ppeers = [of_plane(lax.rem(plane + k, 32)) for k in range(1, 32)]
    zlow, zhigh = at(gz=lax.rem(gz + ngz - 1, ngz)), at(gz=lax.rem(gz + 1, ngz))
    xlow, xhigh = at(gx=lax.rem(gx + ngx - 1, ngx)), at(gx=lax.rem(gx + 1, ngx))

    barrier = pltpu.get_barrier_semaphore()
    yprev, ynext = of_z(zabs, -1), of_z(zabs, 1)
    other = at(gz=zlo * 2 + 1 - core)
    outer_far = (gz == 0) | (gz == ngz - 1)
    outer = at(gz=lax.rem(gz + ngz - 1 + 2 * core, ngz))
    across_z = lax.rem(zabs + 19 - 6 * core, 16)
    across = at(gz=lax.rem(across_z, 8) * 2 + 1 - core, gy=y * 2 + across_z // 8)
    nearest = [of_z(zabs + 16 + k) for k in (-4, 4, -3, 3, -2, 2, -1, 1)]
    below, above = nearest[:2]
    nearest += [of_z(zabs + 4, 1), of_z(zabs + 12, -1), across]
    nearest += [xlow, xhigh, yprev, ynext, other]
    for d in nearest:
        pl.semaphore_signal(barrier, inc=1, device_id=d, device_id_type=MESH)

    @pl.when(jnp.logical_not(outer_far))
    def _():
        pl.semaphore_signal(barrier, inc=1, device_id=outer, device_id_type=MESH)

    loads = [
        pltpu.make_async_copy(vel_h, V.at[pl.ds(0, 3), pl.ds(BY, ROWS), :], lsem.at[0]),
        pltpu.make_async_copy(pres_h, V.at[3, pl.ds(BY, ROWS), :], lsem.at[1]),
        pltpu.make_async_copy(eps_h, E, lsem.at[2]),
        pltpu.make_async_copy(pv_h, PV, lsem.at[3]),
        pltpu.make_async_copy(force_h, scal.at[0], lsem.at[4]),
        pltpu.make_async_copy(target_h, scal.at[1], lsem.at[5]),
    ]
    for cp in loads:
        cp.start()

    lane = lax.broadcasted_iota(jnp.int32, (BY, BZ), 1)
    rown = lax.broadcasted_iota(jnp.int32, (BY, BZ), 0)
    zero = jnp.zeros((BY, BZ), jnp.float32)
    for f in range(4):
        V[f, pl.ds(0, BY), :] = zero
        V[f, pl.ds(ROWS + BY, BY), :] = zero
    Q[...] = jnp.zeros_like(Q)
    for cp in loads:
        cp.wait()
    force, target = scal[0, 0], scal[1, 0]

    def face(side):
        return 0 if side == 0 else BY - 1

    for side in range(2):
        rows = pl.ds(face(side), BX, stride=BY)
        v = [V[f, pl.ds(BY + face(side), BX, stride=BY), :] for f in range(4)]
        ysend[side, FVZ], ysend[side, FVY] = v[VZ], v[VY]
        ysend[side, FP], ysend[side, FVX] = v[PR], v[VX]
        e = E[rows, :]
        ysend[side, FD] = e * DT * weight(v, [PV[k, rows, :] for k in range(3)], e)[1]

    def remote(src, dst, a, b, dev):
        return pltpu.make_async_remote_copy(
            src_ref=src, dst_ref=dst, send_sem=a, recv_sem=b, device_id=dev, device_id_type=MESH
        )

    def side_of(kind):
        return 1 - zhi if kind == 0 else zhi

    def ycopy(kind, j):
        side, part = side_of(kind), pl.ds(*GROUPS[j])
        return remote(
            ysend.at[side, part], mrecv.at[1 - side, part], ys.at[kind, j], mr.at[1 - side, j],
            of_z(zabs + 12 + 8 * side, kind * zhi),
        )

    def paired(kind):
        return (gy >= 0) if kind == 0 else jnp.where(zhi == 0, y, 3 - y) > 0

    def mwait(q, j):
        part = pl.ds(*GROUPS[j])
        remote(ysend.at[0, part], mrecv.at[q, part], ys.at[0, j], mr.at[q, j], above).wait_recv()

    def yhas(side):
        return has_ylo if side == 0 else has_yhi

    intra = (zabs >= 4) & (zabs < 12)
    middle = intra | (y > 0)

    def mcopy(q, j):
        part = pl.ds(*BACK[j])
        return remote(
            msend.at[q, part], yrecv.at[1 - q, part], ms.at[q, j], yr.at[1 - q, j],
            of_z(zabs + 12, jnp.where(intra, 0, -1)) if q == 0 else of_z(zabs + 4),
        )

    def xcopy(side):
        r = BY if side == 0 else ROWS
        return remote(
            V.at[:, pl.ds(r, BY), :], xrecv.at[1 - side], xs.at[side], xr.at[1 - side],
            xlow if side == 0 else xhigh,
        )

    def xhas(side):
        return has_xlo if side == 0 else has_xhi

    def zcopy(side, src, dst, a, b):
        return remote(
            src.at[side], dst.at[1 - side], a.at[side], b.at[1 - side],
            zlow if side == 0 else zhigh,
        )

    def when_each(has, fn):
        for side in range(2):
            pl.when(has(side))(lambda side=side: fn(side))

    def send_y(kind, groups):
        @pl.when(paired(kind))
        def _():
            for g in groups:
                ycopy(kind, g).start()

    def heard():
        pl.semaphore_wait(know.at[0], 1)
        pl.semaphore_wait(know.at[1], 1)

    waves = [(xlow, xhigh), (yprev, ynext), (yprev, ynext), (other,)]

    def plane_tell(i):
        for d in waves[i]:
            pl.semaphore_signal(wave.at[i], inc=1, device_id=d, device_id_type=MESH)

    def plane_heard(i):
        pl.semaphore_wait(wave.at[i], len(waves[i]))

    def columns(x, carry):
        o = pl.multiple_of(x * BY, BY)
        s = zero
        for k, a in enumerate([V[f, pl.ds(o + BY, BY), :] for f in range(4)] + [E[pl.ds(o, BY), :]]):
            s = jnp.where(lane == k, a if k == 0 else pltpu.roll(a, k, 1), s)
            s = jnp.where(lane == 8 + k, pltpu.roll(a, 9 + k, 1), s)
        S[pl.ds(o, BY), :] = s
        return carry

    lax.fori_loop(0, BX, columns, 0, unroll=4)

    def pack(dst, n):
        for i in range(4):
            t = S[pl.ds(BZ * i, BZ), :].T
            for k in range(n):
                dst[0, k, :, pl.ds(BZ * i, BZ)] = t[k:k + 1]
                dst[1, k, :, pl.ds(BZ * i, BZ)] = t[8 + k:9 + k]

    pack(zsend, 5)
    relay = zlo == 4 - core

    def zwrap():
        return remote(
            zsend.at[core], rbuf, zs.at[core], rsem, of_z(zabs + 20 - 8 * core),
        )

    def zforward():
        return remote(
            rbuf, zrecv.at[1 - core], fsem, zr.at[1 - core], at(gz=gz + 7 - 14 * core),
        )

    pl.semaphore_wait(barrier, len(nearest) + jnp.where(outer_far, 0, 1))
    @pl.when(outer_far)
    def _():
        zwrap().start()

    for side in range(2):
        @pl.when(jnp.logical_not(outer_far & (core == side)))
        def _():
            zcopy(side, zsend, zrecv, zs, zr).start()

    send_y(0, (0,))
    send_y(1, (0,))
    when_each(xhas, lambda side: xcopy(side).start())

    pl.semaphore_signal(know.at[0], inc=1, device_id=above, device_id_type=MESH)
    pl.semaphore_signal(know.at[1], inc=1, device_id=below, device_id_type=MESH)
    plane_tell(0)

    def slab(x, carry):
        o = pl.multiple_of(x * BY, BY)
        c = [V[f, pl.ds(o + BY, BY), :] for f in range(4)]
        xm = [V[f, pl.ds(o, BY), :] for f in range(4)]
        xp = [V[f, pl.ds(o + 2 * BY, BY), :] for f in range(4)]
        e = E[pl.ds(o, BY), :]
        pv = [PV[k, pl.ds(o, BY), :] for k in range(3)]
        zm = [jnp.where(lane == 0, 0.0, pltpu.roll(a, 1, 1)) for a in c]
        zp = [jnp.where(lane == BZ - 1, 0.0, pltpu.roll(a, BZ - 1, 1)) for a in c]
        ym = [jnp.where(rown == 0, 0.0, pltpu.roll(a, 1, 0)) for a in c]
        yp = [jnp.where(rown == BY - 1, 0.0, pltpu.roll(a, BY - 1, 0)) for a in c]
        drag, w = weight(c, pv, e)
        hi, lo = (xp, yp, zp), (xm, ym, zm)
        for k in range(3):
            adv = zero
            lap = -6.0 * c[k]
            for d in range(3):
                adv = adv + c[d] * (hi[d][k] - lo[d][k])
                lap = lap + hi[d][k] + lo[d][k]
            fk = NU * lap - 0.5 * (adv + (hi[k][3] - lo[k][3]))
            if k == 2:
                fk = fk + force
            vel_o[k, pl.ds(o, BY), :] = (c[k] + DT * (fk + drag * pv[k])) * w
        G[pl.ds(o, BY), :] = DT * w
        return carry

    lax.fori_loop(0, BX, slab, 0, unroll=4)
    plane_heard(0)
    plane_tell(1)

    @pl.when(outer_far)
    def _():
        send_y(0, (1,))
        send_y(1, (1,))

    @pl.when(relay)
    def _():
        zwrap().wait_recv()
        zforward().start()

    plane_heard(1)
    plane_tell(2)

    def not_(has):
        return lambda side: jnp.logical_not(has(side))

    def wall_y(side):
        sg = 0.5 if side == 0 else -0.5
        for f in (NZ_, NX_, NF_):
            yrecv[side, f] = jnp.zeros((BX, BZ), jnp.float32)
        yrecv[side, NY_] = sg * ysend[side, FP]

    def wall_x(side):
        for f in (VX, VY, VZ):
            xrecv[side, f] = zero
        xrecv[side, PR] = V[PR, pl.ds(BY if side == 0 else ROWS, BY), :]
        FX[pl.ds(0 if side == 0 else ROWS + BY, BY), :] = zero

    when_each(not_(yhas), wall_y)
    when_each(not_(xhas), wall_x)

    when_each(xhas, lambda side: xcopy(1 - side).wait_recv())
    for side in range(2):
        sg = 0.5 if side == 0 else -0.5
        r = BY if side == 0 else ROWS
        g = G[pl.ds(r - BY, BY), :]
        coef = NU + sg * V[VX, pl.ds(r, BY), :]
        for k in range(3):
            n = coef * xrecv[side, k]
            if k == 0:
                n = n + sg * xrecv[side, PR]
            vel_o[k, pl.ds(r - BY, BY), :] += g * n

    for side in range(2):
        zcopy(1 - side, zsend, zrecv, zs, zr).wait_recv()
    for i in range(4):
        ln = pl.ds(BZ * i, BZ)
        vlo, vhi = zsend[0, 2, :, ln], zsend[1, 2, :, ln]
        clo, chi = NU + 0.5 * vlo, NU - 0.5 * vhi
        for k in range(3):
            nlo, nhi = clo * zrecv[0, k, :, ln], chi * zrecv[1, k, :, ln]
            if k == 2:
                nlo = nlo + 0.5 * zrecv[0, 3, :, ln]
                nhi = nhi - 0.5 * zrecv[1, 3, :, ln]
            Q[2 * k:2 * k + 1, ln] = nhi
            Q[2 * k + 1:2 * k + 2, ln] = nlo
        Q[6:7, ln] = zrecv[1, 4, :, ln]
        Q[7:8, ln] = zrecv[0, 4, :, ln]

    def unpack():
        for i in range(4):
            S[pl.ds(BZ * i, BZ), :] = Q[:, pl.ds(BZ * i, BZ)].T

    unpack()
    edge = (lane == 0) | (lane == BZ - 1)

    def zfix(x, carry):
        flow, void = carry
        o = pl.multiple_of(x * BY, BY)
        q, g, e = S[pl.ds(o, BY), :], G[pl.ds(o, BY), :], E[pl.ds(o, BY), :]
        for k in range(3):
            u = vel_o[k, pl.ds(o, BY), :] + g * jnp.where(edge, pltpu.roll(q, BZ - 1 - 2 * k, 1), 0.0)
            vel_o[k, pl.ds(o, BY), :] = u
        h = pltpu.roll(q, BZ - 7, 1)
        SL[pl.ds(o, BY), :] = 0.5 * (
            jnp.where(lane == BZ - 1, h, pltpu.roll(e, BZ - 1, 1))
            - jnp.where(lane == 0, h, pltpu.roll(e, 1, 1))
        )
        return flow + e * u, void + e

    flow, void = lax.fori_loop(0, BX, zfix, (zero, zero), unroll=4)

    for side in range(2):
        rows = pl.ds(face(side), BX, stride=BY)
        ysend[side, FC] = E[rows, :] * vel_o[VY, rows, :]
    plane_heard(2)
    plane_tell(3)

    @pl.when(jnp.logical_not(outer_far))
    def _():
        send_y(0, (1,))
        send_y(1, (1,))

    send_y(0, (2,))
    send_y(1, (2,))

    yacc[...] = jnp.zeros_like(yacc)

    def couple(k, f, n):
        for q in range(2):
            sg = -0.5 if q == 0 else 0.5
            t = (NU + sg * mrecv[q, FVY]) * mrecv[1 - q, f]
            if k == VY:
                t = t + sg * mrecv[1 - q, FP]
            msend[q, n] = t

    def both(fn):
        for q in range(2):
            fn(q)

    @pl.when(middle)
    def _():
        both(lambda q: mwait(q, 0))
        couple(VZ, FVZ, NZ_)
        yacc[...] = mrecv[0, FD] * msend[0, NZ_] + mrecv[1, FD] * msend[1, NZ_]

    def spread(a, b):
        a, b = jnp.sum(a, axis=0, keepdims=True), jnp.sum(b, axis=0, keepdims=True)
        return jnp.where(
            lane[0:1] < BZ // 2, a + pltpu.roll(a, BZ // 2, 1), b + pltpu.roll(b, BZ // 2, 1)
        )

    part = spread(flow + (yacc[0:16] + yacc[16:32]), void)
    row1[0] = part
    red1[zabs] = part

    def c1(k):
        return remote(row1.at[0], red1.at[zabs], s1, r1, zpeers[k - 1])

    def c2(k):
        return remote(row2.at[0], red2.at[plane], s2, r2, ppeers[k - 1])

    heard()
    for k in range(1, 16):
        c1(k).start()

    @pl.when(middle)
    def _():
        both(lambda q: mcopy(q, 0).start())
        both(lambda q: mwait(q, 1))
        couple(VY, FVY, NY_)
        couple(VX, FVX, NX_)
        both(lambda q: mcopy(q, 1).start())

    @pl.when(middle)
    def _():
        both(lambda q: mwait(q, 2))
        for q in range(2):
            msend[q, NF_] = mrecv[1 - q, FC] + mrecv[1 - q, FD] * msend[1 - q, NY_]
        both(lambda q: mcopy(q, 2).start())

    def yback(j, terms):
        when_each(yhas, lambda side: mcopy(1 - side, j).wait_recv())
        for side in range(2):
            rows = pl.ds(face(side), BX, stride=BY)
            g = G[rows, :]
            for k, n in terms:
                vel_o[k, rows, :] = vel_o[k, rows, :] + g * yrecv[side, n]

    def zstep():
        yback(0, ((VZ, NZ_),))

        def zflux(x, carry):
            o = pl.multiple_of(x * BY, BY)
            fz = E[pl.ds(o, BY), :] * vel_o[VZ, pl.ds(o, BY), :]
            S[pl.ds(o, BY), :] = jnp.where(lane == 8, pltpu.roll(fz, 9, 1), fz)
            return carry

        lax.fori_loop(0, BX, zflux, 0, unroll=8)
        pack(zsend2, 1)
        for side in range(2):
            zcopy(side, zsend2, zrecv2, zs2, zr2).start()

    pl.when(gz == ngz - 1)(zstep)

    def all_of(red, n, a, b):
        return remote(red.at[pl.ds(0, n)], red.at[pl.ds(0, n)], a, b, above)

    all_of(red1, 15, s1, r1).wait_recv()
    part2 = red1[0]
    for i in range(1, 16):
        part2 = part2 + red1[i]
    row2[0] = part2
    red2[plane] = part2
    plane_heard(3)
    for k in range(1, 32):
        c2(k).start()

    pl.when(gz < ngz - 1)(zstep)

    yback(1, ((VX, NX_), (VY, NY_)))

    def xflux(x, carry):
        o = pl.multiple_of(x * BY, BY)
        FX[pl.ds(o + BY, BY), :] = E[pl.ds(o, BY), :] * vel_o[VX, pl.ds(o, BY), :]
        return carry

    lax.fori_loop(0, BX, xflux, 0, unroll=8)
    for side in range(2):
        xsend2[side] = FX[pl.ds(BY if side == 0 else ROWS, BY), :]

    def xcopy2(side):
        return remote(
            xsend2.at[side], FX.at[pl.ds(ROWS + BY if side == 0 else 0, BY), :],
            xs2.at[side], xr2.at[1 - side], xlow if side == 0 else xhigh,
        )

    when_each(xhas, lambda side: xcopy2(side).start())

    when_each(yhas, lambda side: mcopy(1 - side, 2).wait_recv())
    when_each(xhas, lambda side: xcopy2(1 - side).wait_recv())

    def diverge(x, carry):
        o = pl.multiple_of(x * BY, BY)
        e = E[pl.ds(o, BY), :]
        fy = e * vel_o[VY, pl.ds(o, BY), :]
        fz = e * vel_o[VZ, pl.ds(o, BY), :]
        d = FX[pl.ds(o + 2 * BY, BY), :] - FX[pl.ds(o, BY), :]
        d = d + (
            jnp.where(rown == BY - 1, yrecv[1, NF_, pl.ds(x, 1), :], pltpu.roll(fy, BY - 1, 0))
            - jnp.where(rown == 0, yrecv[0, NF_, pl.ds(x, 1), :], pltpu.roll(fy, 1, 0))
        )
        d = d + (
            jnp.where(lane == BZ - 1, 0.0, pltpu.roll(fz, BZ - 1, 1))
            - jnp.where(lane == 0, 0.0, pltpu.roll(fz, 1, 1))
        )
        src_o[pl.ds(o, BY), :] = 0.5 * d
        return carry

    lax.fori_loop(0, BX, diverge, 0, unroll=4)

    for side in range(2):
        zcopy(1 - side, zsend2, zrecv2, zs2, zr2).wait_recv()
    Q[0:1, :] = zrecv2[1, 0]
    Q[1:2, :] = zrecv2[0, 0]
    unpack()
    all_of(red2, 31, s2, r2).wait_recv()
    total = red2[0]
    for i in range(1, 32):
        total = total + red2[i]
    half = lane[0:1] < BZ // 2
    flow_sum = jnp.sum(jnp.where(half, total, 0.0), axis=1, keepdims=True)
    void_sum = jnp.sum(jnp.where(half, 0.0, total), axis=1, keepdims=True)
    cells = float(ROWS * BZ * 512)
    step = (target * cells - flow_sum) / (DT * void_sum)
    aux_o[0:1, :] = jnp.broadcast_to(DT * step, (1, BZ))
    aux_o[1:2, :] = jnp.broadcast_to(force + step, (1, BZ))

    for kind in range(2):
        @pl.when(paired(kind))
        def _():
            for j in range(3):
                ycopy(kind, j).wait_send()

    @pl.when(middle)
    def _():
        both(lambda q: [mcopy(q, j).wait_send() for j in range(3)])

    when_each(xhas, lambda side: (xcopy(side).wait_send(), xcopy2(side).wait_send()) and None)
    @pl.when(relay)
    def _():
        zforward().wait_send()

    for side in range(2):
        zcopy(side, zsend, zrecv, zs, zr).wait_send()
        zcopy(side, zsend2, zrecv2, zs2, zr2).wait_send()
    all_of(red1, 15, s1, r1).wait_send()
    all_of(red2, 31, s2, r2).wait_send()


def finish(vel, src, slope, aux, halo, vel_o, src_o, force_o, vz, out, sem):
    pairs = [
        pltpu.make_async_copy(vel.at[pl.ds(0, 2)], vel_o.at[pl.ds(0, 2)], sem.at[0]),
        pltpu.make_async_copy(vz, vel_o.at[VZ], sem.at[1]),
        pltpu.make_async_copy(out, src_o, sem.at[2]),
    ]
    pairs[0].start()
    force_o[...] = aux[1:2, 0:1]
    add = aux[0:1, :]
    vz[...] = vel[VZ] + add
    pairs[1].start()
    lane = lax.broadcasted_iota(jnp.int32, (ROWS, BZ), 1)
    sign = jnp.where(lane == 0, -0.5, jnp.where(lane == BZ - 1, 0.5, 0.0))
    out[...] = src[...] + add * slope[...] + sign * pltpu.roll(halo[...], BZ - 1, 1)
    pairs[2].start()
    for cp in pairs:
        cp.wait()


def local(velocity, pressure, voidage, particle_vel, forcing, target_flux):
    f32 = jnp.float32
    vmem = pl.BlockSpec(memory_space=pltpu.VMEM)
    hbm = pl.BlockSpec(memory_space=pl.ANY)
    dma = pltpu.SemaphoreType.DMA
    parts = pl.pallas_call(
        kernel,
        out_shape=(
            pltpu.VMEM((3, ROWS, BZ), f32),
            pltpu.VMEM((ROWS, BZ), f32),
            pltpu.VMEM((ROWS, BZ), f32),
            pltpu.VMEM((8, BZ), f32),
            pltpu.VMEM((ROWS, BZ), f32),
        ),
        in_specs=[pl.BlockSpec(memory_space=pltpu.HBM)] * 6,
        out_specs=(vmem,) * 5,
        scratch_shapes=[
            pltpu.VMEM((4, PAD, BZ), f32),
            pltpu.VMEM((ROWS, BZ), f32),
            pltpu.VMEM((3, ROWS, BZ), f32),
            pltpu.VMEM((ROWS, BZ), f32),
            pltpu.VMEM((PAD, BZ), f32),
            pltpu.VMEM((BZ, ROWS), f32),
            pltpu.SMEM((2, 1), f32),
            pltpu.VMEM((2, 4, BY, BZ), f32),
            pltpu.VMEM((2, 5, 1, ROWS), f32),
            pltpu.VMEM((2, 5, 1, ROWS), f32),
            pltpu.VMEM((2, 1, 1, ROWS), f32),
            pltpu.VMEM((2, 1, 1, ROWS), f32),
            pltpu.VMEM((2, 6, BX, BZ), f32),
            pltpu.VMEM((2, 4, BX, BZ), f32),
            pltpu.VMEM((2, 4, BX, BZ), f32),
            pltpu.VMEM((2, 6, BX, BZ), f32),
            pltpu.VMEM((BX, BZ), f32),
            pltpu.VMEM((2, BY, BZ), f32),
            pltpu.VMEM((5, 1, ROWS), f32),
            pltpu.VMEM((1, 1, BZ), f32),
            pltpu.VMEM((16, 1, BZ), f32),
            pltpu.VMEM((1, 1, BZ), f32),
            pltpu.VMEM((32, 1, BZ), f32),
            dma((6,)), dma((2,)), dma((2,)), dma((2,)), dma((2,)), dma((2,)), dma((2,)),
            dma((2, 3)), dma((2, 3)), dma((2, 3)), dma((2, 3)), dma((2,)), dma((2,)),
            dma, dma, dma, dma, pltpu.SemaphoreType.REGULAR((2,)), pltpu.SemaphoreType.REGULAR((4,)), dma, dma,
        ],
        compiler_params=pltpu.CompilerParams(collective_id=0, has_side_effects=True),
    )(
        forcing,
        target_flux,
        velocity.reshape(3, ROWS, BZ),
        pressure.reshape(ROWS, BZ),
        voidage.reshape(ROWS, BZ),
        particle_vel.reshape(3, ROWS, BZ),
    )
    vel, src, force = pl.pallas_call(
        finish,
        out_shape=(
            jax.ShapeDtypeStruct((3, ROWS, BZ), f32),
            jax.ShapeDtypeStruct((ROWS, BZ), f32),
            jax.ShapeDtypeStruct((1, 1), f32),
        ),
        in_specs=[vmem] * 5,
        out_specs=(hbm, hbm, vmem),
        scratch_shapes=[pltpu.VMEM((ROWS, BZ), f32), pltpu.VMEM((ROWS, BZ), f32), dma((3,))],
        compiler_params=pltpu.CompilerParams(vmem_limit_bytes=8 * 1024 * 1024),
    )(*[pltpu.with_memory_space_constraint(p, pltpu.VMEM) for p in parts])
    return vel.reshape(3, BX, BY, BZ), src.reshape(BX, BY, BZ), force.reshape(1)


def solution(mesh):
    return jax.shard_map(
        local,
        mesh=mesh,
        in_specs=(
            P(None, "gx", "gy", "gz"), P("gx", "gy", "gz"), P("gx", "gy", "gz"),
            P(None, "gx", "gy", "gz"), P(), P(),
        ),
        out_specs=(P(None, "gx", "gy", "gz"), P("gx", "gy", "gz"), P()),
        check_vma=False,
    )
```

```python
import jax
import jax.numpy as jnp
from jax import lax
from jax.experimental import pallas as pl
from jax.experimental.pallas import tpu as pltpu
from jax.sharding import PartitionSpec as P

MESH = pl.DeviceIdType.MESH
DT = 0.2
NU = 0.1
BX, BY, BZ = 32, 16, 128
ROWS = BX * BY
PAD = ROWS + 2 * BY
VX, VY, VZ, PR = 0, 1, 2, 3
FVZ, FVY, FD, FP, FVX, FC = 0, 1, 2, 3, 4, 5
GROUPS = ((0, 3), (3, 2), (5, 1))
NZ_, NY_, NX_, NF_ = 0, 1, 2, 3
BACK = ((0, 1), (1, 2), (3, 1))


def weight(c, pv, e):
    a, b, d = c[0] - pv[0], c[1] - pv[1], c[2] - pv[2]
    slip = jnp.sqrt(a * a + b * b + d * d)
    drag = (1.0 - e) * jnp.exp(-2.65 * jnp.log(e)) * (1.0 + slip)
    return drag, 1.0 / (1.0 + DT * drag)


def kernel(
    force_h, target_h, vel_h, pres_h, eps_h, pv_h,
    vel_o, src_o, SL, aux_o, S,
    V, E, PV, G, FX, Q, scal,
    xrecv, zsend, zrecv, zsend2, zrecv2, ysend, yrecv, msend, mrecv, yacc, xsend2, rbuf,
    row1, red1, row2, red2,
    lsem, xs, xr, zs, zr, zs2, zr2, ys, yr, ms, mr, xs2, xr2, s1, r1, s2, r2, know, wave, rsem, fsem,
):
    gz, gy, gx = lax.axis_index("gz"), lax.axis_index("gy"), lax.axis_index("gx")
    ngz, ngy, ngx = 16, 8, 4
    here = {"gz": gz, "gy": gy, "gx": gx}

    def at(**kw):
        return {**here, **kw}

    y, zhi = gy // 2, gy % 2
    zlo, core = gz // 2, gz % 2
    zabs = zhi * 8 + zlo
    xi, yi = gx, y
    has_xlo, has_xhi = gx > 0, gx < ngx - 1
    has_ylo, has_yhi = gy > 0, gy < ngy - 1

    def of_z(z, dy=0):
        z, yy = lax.rem(z, 16), lax.rem(y + dy + 4, 4)
        return at(gz=lax.rem(z, 8) * 2 + core, gy=yy * 2 + z // 8)

    def of_plane(i):
        return at(gx=i // 8, gy=lax.rem(i // 2, 4) * 2 + zhi, gz=zlo * 2 + lax.rem(i, 2))

    plane = gx * 8 + y * 2 + core
    zpeers = [of_z(zabs + k) for k in range(1, 16)]
    ppeers = [of_plane(lax.rem(plane + k, 32)) for k in range(1, 32)]
    zlow, zhigh = at(gz=lax.rem(gz + ngz - 1, ngz)), at(gz=lax.rem(gz + 1, ngz))
    xlow, xhigh = at(gx=lax.rem(gx + ngx - 1, ngx)), at(gx=lax.rem(gx + 1, ngx))

    barrier = pltpu.get_barrier_semaphore()
    yprev, ynext = of_z(zabs, -1), of_z(zabs, 1)
    other = at(gz=zlo * 2 + 1 - core)
    outer_far = (gz == 0) | (gz == ngz - 1)
    outer = at(gz=lax.rem(gz + ngz - 1 + 2 * core, ngz))
    across_z = lax.rem(zabs + 19 - 6 * core, 16)
    across = at(gz=lax.rem(across_z, 8) * 2 + 1 - core, gy=y * 2 + across_z // 8)
    nearest = [of_z(zabs + 16 + k) for k in (-4, 4, -3, 3, -2, 2, -1, 1)]
    below, above = nearest[:2]
    nearest += [of_z(zabs + 4, 1), of_z(zabs + 12, -1), across]
    nearest += [xlow, xhigh, yprev, ynext, other]
    for d in nearest:
        pl.semaphore_signal(barrier, inc=1, device_id=d, device_id_type=MESH)

    @pl.when(jnp.logical_not(outer_far))
    def _():
        pl.semaphore_signal(barrier, inc=1, device_id=outer, device_id_type=MESH)

    loads = [
        pltpu.make_async_copy(vel_h, V.at[pl.ds(0, 3), pl.ds(BY, ROWS), :], lsem.at[0]),
        pltpu.make_async_copy(pres_h, V.at[3, pl.ds(BY, ROWS), :], lsem.at[1]),
        pltpu.make_async_copy(eps_h, E, lsem.at[2]),
        pltpu.make_async_copy(pv_h, PV, lsem.at[3]),
        pltpu.make_async_copy(force_h, scal.at[0], lsem.at[4]),
        pltpu.make_async_copy(target_h, scal.at[1], lsem.at[5]),
    ]
    for cp in loads:
        cp.start()

    lane = lax.broadcasted_iota(jnp.int32, (BY, BZ), 1)
    rown = lax.broadcasted_iota(jnp.int32, (BY, BZ), 0)
    zero = jnp.zeros((BY, BZ), jnp.float32)
    for f in range(4):
        V[f, pl.ds(0, BY), :] = zero
        V[f, pl.ds(ROWS + BY, BY), :] = zero
    Q[...] = jnp.zeros_like(Q)
    for cp in loads:
        cp.wait()
    force, target = scal[0, 0], scal[1, 0]

    def face(side):
        return 0 if side == 0 else BY - 1

    for side in range(2):
        rows = pl.ds(face(side), BX, stride=BY)
        v = [V[f, pl.ds(BY + face(side), BX, stride=BY), :] for f in range(4)]
        ysend[side, FVZ], ysend[side, FVY] = v[VZ], v[VY]
        ysend[side, FP], ysend[side, FVX] = v[PR], v[VX]
        e = E[rows, :]
        ysend[side, FD] = e * DT * weight(v, [PV[k, rows, :] for k in range(3)], e)[1]

    def remote(src, dst, a, b, dev):
        return pltpu.make_async_remote_copy(
            src_ref=src, dst_ref=dst, send_sem=a, recv_sem=b, device_id=dev, device_id_type=MESH
        )

    def side_of(kind):
        return 1 - zhi if kind == 0 else zhi

    def ycopy(kind, j):
        side, part = side_of(kind), pl.ds(*GROUPS[j])
        return remote(
            ysend.at[side, part], mrecv.at[1 - side, part], ys.at[kind, j], mr.at[1 - side, j],
            of_z(zabs + 12 + 8 * side, kind * zhi),
        )

    def paired(kind):
        return (gy >= 0) if kind == 0 else jnp.where(zhi == 0, y, 3 - y) > 0

    def mwait(q, j):
        part = pl.ds(*GROUPS[j])
        remote(ysend.at[0, part], mrecv.at[q, part], ys.at[0, j], mr.at[q, j], above).wait_recv()

    def yhas(side):
        return has_ylo if side == 0 else has_yhi

    intra = (zabs >= 4) & (zabs < 12)
    middle = intra | (y > 0)

    def mcopy(q, j):
        part = pl.ds(*BACK[j])
        return remote(
            msend.at[q, part], yrecv.at[1 - q, part], ms.at[q, j], yr.at[1 - q, j],
            of_z(zabs + 12, jnp.where(intra, 0, -1)) if q == 0 else of_z(zabs + 4),
        )

    def xcopy(side):
        r = BY if side == 0 else ROWS
        return remote(
            V.at[:, pl.ds(r, BY), :], xrecv.at[1 - side], xs.at[side], xr.at[1 - side],
            xlow if side == 0 else xhigh,
        )

    def xhas(side):
        return has_xlo if side == 0 else has_xhi

    def zcopy(side, src, dst, a, b):
        return remote(
            src.at[side], dst.at[1 - side], a.at[side], b.at[1 - side],
            zlow if side == 0 else zhigh,
        )

    def when_each(has, fn):
        for side in range(2):
            pl.when(has(side))(lambda side=side: fn(side))

    def send_y(kind, groups):
        @pl.when(paired(kind))
        def _():
            for g in groups:
                ycopy(kind, g).start()

    def heard():
        pl.semaphore_wait(know.at[0], 1)
        pl.semaphore_wait(know.at[1], 1)

    waves = [(xlow, xhigh), (yprev, ynext), (yprev, ynext), (other,)]

    def plane_tell(i):
        for d in waves[i]:
            pl.semaphore_signal(wave.at[i], inc=1, device_id=d, device_id_type=MESH)

    def plane_heard(i):
        pl.semaphore_wait(wave.at[i], len(waves[i]))

    def columns(x, carry):
        o = pl.multiple_of(x * BY, BY)
        s = zero
        for k, a in enumerate([V[f, pl.ds(o + BY, BY), :] for f in range(4)] + [E[pl.ds(o, BY), :]]):
            s = jnp.where(lane == k, a if k == 0 else pltpu.roll(a, k, 1), s)
            s = jnp.where(lane == 8 + k, pltpu.roll(a, 9 + k, 1), s)
        S[pl.ds(o, BY), :] = s
        return carry

    lax.fori_loop(0, BX, columns, 0, unroll=2)

    def pack(dst, n):
        for i in range(4):
            t = S[pl.ds(BZ * i, BZ), :].T
            for k in range(n):
                dst[0, k, :, pl.ds(BZ * i, BZ)] = t[k:k + 1]
                dst[1, k, :, pl.ds(BZ * i, BZ)] = t[8 + k:9 + k]

    pack(zsend, 5)
    relay = zlo == 4 - core

    def zwrap():
        return remote(
            zsend.at[core], rbuf, zs.at[core], rsem, of_z(zabs + 20 - 8 * core),
        )

    def zforward():
        return remote(
            rbuf, zrecv.at[1 - core], fsem, zr.at[1 - core], at(gz=gz + 7 - 14 * core),
        )

    pl.semaphore_wait(barrier, len(nearest) + jnp.where(outer_far, 0, 1))
    @pl.when(outer_far)
    def _():
        zwrap().start()

    for side in range(2):
        @pl.when(jnp.logical_not(outer_far & (core == side)))
        def _():
            zcopy(side, zsend, zrecv, zs, zr).start()

    send_y(0, (0,))
    send_y(1, (0,))
    when_each(xhas, lambda side: xcopy(side).start())

    pl.semaphore_signal(know.at[0], inc=1, device_id=above, device_id_type=MESH)
    pl.semaphore_signal(know.at[1], inc=1, device_id=below, device_id_type=MESH)
    plane_tell(0)

    def slab(x, carry):
        o = pl.multiple_of(x * BY, BY)
        c = [V[f, pl.ds(o + BY, BY), :] for f in range(4)]
        xm = [V[f, pl.ds(o, BY), :] for f in range(4)]
        xp = [V[f, pl.ds(o + 2 * BY, BY), :] for f in range(4)]
        e = E[pl.ds(o, BY), :]
        pv = [PV[k, pl.ds(o, BY), :] for k in range(3)]
        zm = [jnp.where(lane == 0, 0.0, pltpu.roll(a, 1, 1)) for a in c]
        zp = [jnp.where(lane == BZ - 1, 0.0, pltpu.roll(a, BZ - 1, 1)) for a in c]
        ym = [jnp.where(rown == 0, 0.0, pltpu.roll(a, 1, 0)) for a in c]
        yp = [jnp.where(rown == BY - 1, 0.0, pltpu.roll(a, BY - 1, 0)) for a in c]
        drag, w = weight(c, pv, e)
        hi, lo = (xp, yp, zp), (xm, ym, zm)
        for k in range(3):
            adv = zero
            lap = -6.0 * c[k]
            for d in range(3):
                adv = adv + c[d] * (hi[d][k] - lo[d][k])
                lap = lap + hi[d][k] + lo[d][k]
            fk = NU * lap - 0.5 * (adv + (hi[k][3] - lo[k][3]))
            if k == 2:
                fk = fk + force
            vel_o[k, pl.ds(o, BY), :] = (c[k] + DT * (fk + drag * pv[k])) * w
        G[pl.ds(o, BY), :] = DT * w
        return carry

    lax.fori_loop(0, BX, slab, 0, unroll=4)
    plane_heard(0)
    plane_tell(1)

    @pl.when(outer_far)
    def _():
        send_y(0, (1,))
        send_y(1, (1,))

    @pl.when(relay)
    def _():
        zwrap().wait_recv()
        zforward().start()

    plane_heard(1)
    plane_tell(2)

    def not_(has):
        return lambda side: jnp.logical_not(has(side))

    def wall_y(side):
        sg = 0.5 if side == 0 else -0.5
        for f in (NZ_, NX_, NF_):
            yrecv[side, f] = jnp.zeros((BX, BZ), jnp.float32)
        yrecv[side, NY_] = sg * ysend[side, FP]

    def wall_x(side):
        for f in (VX, VY, VZ):
            xrecv[side, f] = zero
        xrecv[side, PR] = V[PR, pl.ds(BY if side == 0 else ROWS, BY), :]
        FX[pl.ds(0 if side == 0 else ROWS + BY, BY), :] = zero

    when_each(not_(yhas), wall_y)
    when_each(not_(xhas), wall_x)

    when_each(xhas, lambda side: xcopy(1 - side).wait_recv())
    for side in range(2):
        sg = 0.5 if side == 0 else -0.5
        r = BY if side == 0 else ROWS
        g = G[pl.ds(r - BY, BY), :]
        coef = NU + sg * V[VX, pl.ds(r, BY), :]
        for k in range(3):
            n = coef * xrecv[side, k]
            if k == 0:
                n = n + sg * xrecv[side, PR]
            vel_o[k, pl.ds(r - BY, BY), :] += g * n

    for side in range(2):
        zcopy(1 - side, zsend, zrecv, zs, zr).wait_recv()
    for i in range(4):
        ln = pl.ds(BZ * i, BZ)
        vlo, vhi = zsend[0, 2, :, ln], zsend[1, 2, :, ln]
        clo, chi = NU + 0.5 * vlo, NU - 0.5 * vhi
        for k in range(3):
            nlo, nhi = clo * zrecv[0, k, :, ln], chi * zrecv[1, k, :, ln]
            if k == 2:
                nlo = nlo + 0.5 * zrecv[0, 3, :, ln]
                nhi = nhi - 0.5 * zrecv[1, 3, :, ln]
            Q[2 * k:2 * k + 1, ln] = nhi
            Q[2 * k + 1:2 * k + 2, ln] = nlo
        Q[6:7, ln] = zrecv[1, 4, :, ln]
        Q[7:8, ln] = zrecv[0, 4, :, ln]

    def unpack():
        for i in range(4):
            S[pl.ds(BZ * i, BZ), :] = Q[:, pl.ds(BZ * i, BZ)].T

    unpack()
    edge = (lane == 0) | (lane == BZ - 1)

    def zfix(x, carry):
        flow, void = carry
        o = pl.multiple_of(x * BY, BY)
        q, g, e = S[pl.ds(o, BY), :], G[pl.ds(o, BY), :], E[pl.ds(o, BY), :]
        for k in range(3):
            u = vel_o[k, pl.ds(o, BY), :] + g * jnp.where(edge, pltpu.roll(q, BZ - 1 - 2 * k, 1), 0.0)
            vel_o[k, pl.ds(o, BY), :] = u
        h = pltpu.roll(q, BZ - 7, 1)
        SL[pl.ds(o, BY), :] = 0.5 * (
            jnp.where(lane == BZ - 1, h, pltpu.roll(e, BZ - 1, 1))
            - jnp.where(lane == 0, h, pltpu.roll(e, 1, 1))
        )
        return flow + e * u, void + e

    flow, void = lax.fori_loop(0, BX, zfix, (zero, zero), unroll=4)

    for side in range(2):
        rows = pl.ds(face(side), BX, stride=BY)
        ysend[side, FC] = E[rows, :] * vel_o[VY, rows, :]
    plane_heard(2)
    plane_tell(3)

    @pl.when(jnp.logical_not(outer_far))
    def _():
        send_y(0, (1,))
        send_y(1, (1,))

    send_y(0, (2,))
    send_y(1, (2,))

    yacc[...] = jnp.zeros_like(yacc)

    def couple(k, f, n):
        for q in range(2):
            sg = -0.5 if q == 0 else 0.5
            t = (NU + sg * mrecv[q, FVY]) * mrecv[1 - q, f]
            if k == VY:
                t = t + sg * mrecv[1 - q, FP]
            msend[q, n] = t

    def both(fn):
        for q in range(2):
            fn(q)

    @pl.when(middle)
    def _():
        both(lambda q: mwait(q, 0))
        couple(VZ, FVZ, NZ_)
        yacc[...] = mrecv[0, FD] * msend[0, NZ_] + mrecv[1, FD] * msend[1, NZ_]

    def spread(a, b):
        a, b = jnp.sum(a, axis=0, keepdims=True), jnp.sum(b, axis=0, keepdims=True)
        return jnp.where(
            lane[0:1] < BZ // 2, a + pltpu.roll(a, BZ // 2, 1), b + pltpu.roll(b, BZ // 2, 1)
        )

    part = spread(flow + (yacc[0:16] + yacc[16:32]), void)
    row1[0] = part
    red1[zabs] = part

    def c1(k):
        return remote(row1.at[0], red1.at[zabs], s1, r1, zpeers[k - 1])

    def c2(k):
        return remote(row2.at[0], red2.at[plane], s2, r2, ppeers[k - 1])

    heard()
    for k in range(1, 16):
        c1(k).start()

    @pl.when(middle)
    def _():
        both(lambda q: mcopy(q, 0).start())
        both(lambda q: mwait(q, 1))
        couple(VY, FVY, NY_)
        couple(VX, FVX, NX_)
        both(lambda q: mcopy(q, 1).start())

    @pl.when(middle)
    def _():
        both(lambda q: mwait(q, 2))
        for q in range(2):
            msend[q, NF_] = mrecv[1 - q, FC] + mrecv[1 - q, FD] * msend[1 - q, NY_]
        both(lambda q: mcopy(q, 2).start())

    def yback(j, terms):
        when_each(yhas, lambda side: mcopy(1 - side, j).wait_recv())
        for side in range(2):
            rows = pl.ds(face(side), BX, stride=BY)
            g = G[rows, :]
            for k, n in terms:
                vel_o[k, rows, :] = vel_o[k, rows, :] + g * yrecv[side, n]

    def zstep():
        yback(0, ((VZ, NZ_),))

        def zflux(x, carry):
            o = pl.multiple_of(x * BY, BY)
            fz = E[pl.ds(o, BY), :] * vel_o[VZ, pl.ds(o, BY), :]
            S[pl.ds(o, BY), :] = jnp.where(lane == 8, pltpu.roll(fz, 9, 1), fz)
            return carry

        lax.fori_loop(0, BX, zflux, 0, unroll=4)
        pack(zsend2, 1)
        for side in range(2):
            zcopy(side, zsend2, zrecv2, zs2, zr2).start()

    pl.when(gz == ngz - 1)(zstep)

    def all_of(red, n, a, b):
        return remote(red.at[pl.ds(0, n)], red.at[pl.ds(0, n)], a, b, above)

    all_of(red1, 15, s1, r1).wait_recv()
    part2 = red1[0]
    for i in range(1, 16):
        part2 = part2 + red1[i]
    row2[0] = part2
    red2[plane] = part2
    plane_heard(3)
    for k in range(1, 32):
        c2(k).start()

    pl.when(gz < ngz - 1)(zstep)

    yback(1, ((VX, NX_), (VY, NY_)))

    def xflux(x, carry):
        o = pl.multiple_of(x * BY, BY)
        FX[pl.ds(o + BY, BY), :] = E[pl.ds(o, BY), :] * vel_o[VX, pl.ds(o, BY), :]
        return carry

    lax.fori_loop(0, BX, xflux, 0, unroll=4)
    for side in range(2):
        xsend2[side] = FX[pl.ds(BY if side == 0 else ROWS, BY), :]

    def xcopy2(side):
        return remote(
            xsend2.at[side], FX.at[pl.ds(ROWS + BY if side == 0 else 0, BY), :],
            xs2.at[side], xr2.at[1 - side], xlow if side == 0 else xhigh,
        )

    when_each(xhas, lambda side: xcopy2(side).start())

    when_each(yhas, lambda side: mcopy(1 - side, 2).wait_recv())
    when_each(xhas, lambda side: xcopy2(1 - side).wait_recv())

    def diverge(x, carry):
        o = pl.multiple_of(x * BY, BY)
        e = E[pl.ds(o, BY), :]
        fy = e * vel_o[VY, pl.ds(o, BY), :]
        fz = e * vel_o[VZ, pl.ds(o, BY), :]
        d = FX[pl.ds(o + 2 * BY, BY), :] - FX[pl.ds(o, BY), :]
        d = d + (
            jnp.where(rown == BY - 1, yrecv[1, NF_, pl.ds(x, 1), :], pltpu.roll(fy, BY - 1, 0))
            - jnp.where(rown == 0, yrecv[0, NF_, pl.ds(x, 1), :], pltpu.roll(fy, 1, 0))
        )
        d = d + (
            jnp.where(lane == BZ - 1, 0.0, pltpu.roll(fz, BZ - 1, 1))
            - jnp.where(lane == 0, 0.0, pltpu.roll(fz, 1, 1))
        )
        src_o[pl.ds(o, BY), :] = 0.5 * d
        return carry

    lax.fori_loop(0, BX, diverge, 0, unroll=4)

    for side in range(2):
        zcopy(1 - side, zsend2, zrecv2, zs2, zr2).wait_recv()
    Q[0:1, :] = zrecv2[1, 0]
    Q[1:2, :] = zrecv2[0, 0]
    unpack()
    all_of(red2, 31, s2, r2).wait_recv()
    total = red2[0]
    for i in range(1, 32):
        total = total + red2[i]
    half = lane[0:1] < BZ // 2
    flow_sum = jnp.sum(jnp.where(half, total, 0.0), axis=1, keepdims=True)
    void_sum = jnp.sum(jnp.where(half, 0.0, total), axis=1, keepdims=True)
    cells = float(ROWS * BZ * 512)
    step = (target * cells - flow_sum) / (DT * void_sum)
    aux_o[0:1, :] = jnp.broadcast_to(DT * step, (1, BZ))
    aux_o[1:2, :] = jnp.broadcast_to(force + step, (1, BZ))

    for kind in range(2):
        @pl.when(paired(kind))
        def _():
            for j in range(3):
                ycopy(kind, j).wait_send()

    @pl.when(middle)
    def _():
        both(lambda q: [mcopy(q, j).wait_send() for j in range(3)])

    when_each(xhas, lambda side: (xcopy(side).wait_send(), xcopy2(side).wait_send()) and None)
    @pl.when(relay)
    def _():
        zforward().wait_send()

    for side in range(2):
        zcopy(side, zsend, zrecv, zs, zr).wait_send()
        zcopy(side, zsend2, zrecv2, zs2, zr2).wait_send()
    all_of(red1, 15, s1, r1).wait_send()
    all_of(red2, 31, s2, r2).wait_send()


def finish(vel, src, slope, aux, halo, vel_o, src_o, force_o, vz, out, sem):
    pairs = [
        pltpu.make_async_copy(vel.at[pl.ds(0, 2)], vel_o.at[pl.ds(0, 2)], sem.at[0]),
        pltpu.make_async_copy(vz, vel_o.at[VZ], sem.at[1]),
        pltpu.make_async_copy(out, src_o, sem.at[2]),
    ]
    pairs[0].start()
    force_o[...] = aux[1:2, 0:1]
    add = aux[0:1, :]
    vz[...] = vel[VZ] + add
    pairs[1].start()
    lane = lax.broadcasted_iota(jnp.int32, (ROWS, BZ), 1)
    sign = jnp.where(lane == 0, -0.5, jnp.where(lane == BZ - 1, 0.5, 0.0))
    out[...] = src[...] + add * slope[...] + sign * pltpu.roll(halo[...], BZ - 1, 1)
    pairs[2].start()
    for cp in pairs:
        cp.wait()


def local(velocity, pressure, voidage, particle_vel, forcing, target_flux):
    f32 = jnp.float32
    vmem = pl.BlockSpec(memory_space=pltpu.VMEM)
    hbm = pl.BlockSpec(memory_space=pl.ANY)
    dma = pltpu.SemaphoreType.DMA
    parts = pl.pallas_call(
        kernel,
        out_shape=(
            pltpu.VMEM((3, ROWS, BZ), f32),
            pltpu.VMEM((ROWS, BZ), f32),
            pltpu.VMEM((ROWS, BZ), f32),
            pltpu.VMEM((8, BZ), f32),
            pltpu.VMEM((ROWS, BZ), f32),
        ),
        in_specs=[pl.BlockSpec(memory_space=pltpu.HBM)] * 6,
        out_specs=(vmem,) * 5,
        scratch_shapes=[
            pltpu.VMEM((4, PAD, BZ), f32),
            pltpu.VMEM((ROWS, BZ), f32),
            pltpu.VMEM((3, ROWS, BZ), f32),
            pltpu.VMEM((ROWS, BZ), f32),
            pltpu.VMEM((PAD, BZ), f32),
            pltpu.VMEM((BZ, ROWS), f32),
            pltpu.SMEM((2, 1), f32),
            pltpu.VMEM((2, 4, BY, BZ), f32),
            pltpu.VMEM((2, 5, 1, ROWS), f32),
            pltpu.VMEM((2, 5, 1, ROWS), f32),
            pltpu.VMEM((2, 1, 1, ROWS), f32),
            pltpu.VMEM((2, 1, 1, ROWS), f32),
            pltpu.VMEM((2, 6, BX, BZ), f32),
            pltpu.VMEM((2, 4, BX, BZ), f32),
            pltpu.VMEM((2, 4, BX, BZ), f32),
            pltpu.VMEM((2, 6, BX, BZ), f32),
            pltpu.VMEM((BX, BZ), f32),
            pltpu.VMEM((2, BY, BZ), f32),
            pltpu.VMEM((5, 1, ROWS), f32),
            pltpu.VMEM((1, 1, BZ), f32),
            pltpu.VMEM((16, 1, BZ), f32),
            pltpu.VMEM((1, 1, BZ), f32),
            pltpu.VMEM((32, 1, BZ), f32),
            dma((6,)), dma((2,)), dma((2,)), dma((2,)), dma((2,)), dma((2,)), dma((2,)),
            dma((2, 3)), dma((2, 3)), dma((2, 3)), dma((2, 3)), dma((2,)), dma((2,)),
            dma, dma, dma, dma, pltpu.SemaphoreType.REGULAR((2,)), pltpu.SemaphoreType.REGULAR((4,)), dma, dma,
        ],
        compiler_params=pltpu.CompilerParams(collective_id=0, has_side_effects=True),
    )(
        forcing,
        target_flux,
        velocity.reshape(3, ROWS, BZ),
        pressure.reshape(ROWS, BZ),
        voidage.reshape(ROWS, BZ),
        particle_vel.reshape(3, ROWS, BZ),
    )
    vel, src, force = pl.pallas_call(
        finish,
        out_shape=(
            jax.ShapeDtypeStruct((3, ROWS, BZ), f32),
            jax.ShapeDtypeStruct((ROWS, BZ), f32),
            jax.ShapeDtypeStruct((1, 1), f32),
        ),
        in_specs=[vmem] * 5,
        out_specs=(hbm, hbm, vmem),
        scratch_shapes=[pltpu.VMEM((ROWS, BZ), f32), pltpu.VMEM((ROWS, BZ), f32), dma((3,))],
        compiler_params=pltpu.CompilerParams(vmem_limit_bytes=8 * 1024 * 1024),
    )(*[pltpu.with_memory_space_constraint(p, pltpu.VMEM) for p in parts])
    return vel.reshape(3, BX, BY, BZ), src.reshape(BX, BY, BZ), force.reshape(1)


def solution(mesh):
    return jax.shard_map(
        local,
        mesh=mesh,
        in_specs=(
            P(None, "gx", "gy", "gz"), P("gx", "gy", "gz"), P("gx", "gy", "gz"),
            P(None, "gx", "gy", "gz"), P(), P(),
        ),
        out_specs=(P(None, "gx", "gy", "gz"), P("gx", "gy", "gz"), P()),
        check_vma=False,
    )
```
